512 devices in a mesh: grp: 8 (over z), leaf: 64 (over x, y, core).
Axes of the slice: x: 4, y: 8, z: 8, core: 2. Of those that a mesh axis runs over, the one named last changes fastest.
Arguments:
- points: float32 [8, 524288], P(None, ('grp', 'leaf')), may hold values from -6 to 6
- rhs: float32 [16, 524288], P(None, ('grp', 'leaf')), may hold values from -6 to 6
- basis: float32 [524288, 128], P(('grp', 'leaf')), may hold values from -0.1875 to 0.1875
- transfer: float32 [512, 128, 128], P(('grp', 'leaf')), may hold values from -0.5 to 0.5
- noise: float32 [524288], P(('grp', 'leaf')), may hold values from 0.5 to 2
- inv_scale: float32 [8], replicated, may hold values from 0.15 to 0.6
- links: int32 [512, 2], P(('grp', 'leaf')), may hold values from 0 to 1, as said below
- leaf_skel: int32 [512, 128], P(('grp', 'leaf')), may hold values from 0 to 1023, as said below
- group_skel: int32 [8, 128], P('grp'), may hold values from 0 to 8191, as said below
Outputs:
- solution: float32 [16, 524288], P(None, ('grp', 'leaf'))
- residual: float32 [16, 524288], P(None, ('grp', 'leaf'))
The draws below stay inside these ranges and needn't reach their ends.
Inputs may be any that keep to these rules, and one draw needn't show every extreme that they name: `links`: column 1 of box l equals column 0 of box l + 1; column 0 is 0 for the first box of each group of 64 and column 1 for the last. `leaf_skel`: the 128 indices of a box are distinct. `group_skel`: the 128 indices of a group are distinct.
All inputs are finite; a program needn't handle non-finite values.
Results may differ from the reference program's by a relative error of at most 0.0003.
Values sent between devices are 32-bit elements; how exact they have to be, the bound alone decides.
A program may use at most 128 MiB of HBM per device.

```python
import math
import jax
import jax.numpy as jnp
from jax import lax

PTS = 1024
DIM = 8
RHS = 16
SKEL = 128
ITERS = 2
BOXES = 64
GROUPS = 8
LEAVES = 512
NPTS = 524288


def draw_links(key, part):
    raw = jax.random.randint(jax.random.fold_in(key, 11), (LEAVES,), 0, 2)
    place = jnp.arange(LEAVES, dtype=jnp.int32) % BOXES
    upper = jnp.where(place == BOXES - 1, 0, raw)
    lower = jnp.concatenate([jnp.zeros((1,), jnp.int32), upper[:-1]])
    lower = jnp.where(place == 0, 0, lower)
    return jnp.stack([lower, upper], axis=1).astype(jnp.int32)


def draw_leaf_skel(key, part):
    keys = jax.random.split(jax.random.fold_in(key, 23), LEAVES)
    picks = jax.vmap(lambda one: jax.random.permutation(one, PTS)[:SKEL])(keys)
    return picks.astype(jnp.int32)


def draw_group_skel(key, part):
    keys = jax.random.split(jax.random.fold_in(key, 37), GROUPS)
    picks = jax.vmap(lambda one: jax.random.permutation(one, BOXES * SKEL)[:SKEL])(keys)
    return picks.astype(jnp.int32)


def steps_of(own_key, dims, pieces, smallest, top_value):
    level = 1.0
    for dim, parts in pieces:
        steps = jax.random.uniform(jax.random.fold_in(jax.random.fold_in(own_key, 6), dim), (parts,), jnp.float32, smallest / len(pieces), top_value / len(pieces))
        level = level * jnp.repeat(jnp.exp(steps), dims[dim] // parts).reshape((-1,) + (1,) * (len(dims) - 1 - dim))
    return level


def centred(own_key, dims, deviation, bound, cuts=(), kind=jnp.bfloat16):
    entries = jax.random.normal(own_key, dims, jnp.float32) * deviation
    if len(cuts) > 0:
        entries = steps_of(own_key, dims, cuts, -0.22, 0.18) * entries
    return jnp.clip(entries, min=-bound, max=bound).astype(kind)


def setup_inputs(seed: int = 0) -> dict:
    arg_keys = jax.random.split(jax.random.key(seed), 10)
    return {
        "points": centred(arg_keys[0], (DIM, NPTS), 1.0, 6.0, ((1, 512),), jnp.float32),
        "rhs": centred(arg_keys[1], (RHS, NPTS), 1.0, 6.0, ((1, 512),), jnp.float32),
        "basis": centred(arg_keys[2], (NPTS, SKEL), PTS ** -0.5, 0.1875, ((0, 512),), jnp.float32),
        "transfer": centred(arg_keys[3], (LEAVES, SKEL, SKEL), SKEL ** -0.5, 0.5, ((0, 512),), jnp.float32),
        "noise": jnp.clip(jnp.exp(math.log(2.0) - 1.3862944 * jax.random.uniform(arg_keys[4], (NPTS,), jnp.float32) ** steps_of(arg_keys[4], (NPTS,), ((0, 512),), -0.2, 0.2)), 0.5, 2.0),
        "inv_scale": jnp.clip(jnp.exp(jax.random.uniform(arg_keys[5], (DIM,), jnp.float32, math.log(0.15), math.log(0.6))), 0.15, 0.6),
        "links": draw_links(jax.random.fold_in(arg_keys[9], 71), 0),
        "leaf_skel": draw_leaf_skel(jax.random.fold_in(arg_keys[9], 71), 0),
        "group_skel": draw_group_skel(jax.random.fold_in(arg_keys[9], 71), 0),
    }


def kernel_block(left, right, inv_scale):
    first = left * inv_scale[:, None]
    second = right * inv_scale[:, None]
    cross = lax.dot_general(first, second, (((0,), (0,)), ((), ())), precision=lax.Precision.HIGHEST)
    dist = lax.optimization_barrier(jnp.sum(first * first, axis=0))[:, None] + lax.optimization_barrier(jnp.sum(second * second, axis=0))[None, :] - 2.0 * cross
    scaled = jnp.sqrt(5.0 * jnp.maximum(dist, 0.0))
    return (1.0 + scaled + scaled * scaled / 3.0) * jnp.exp(-scaled)

def contract(first, second):
    return lax.dot_general(first, second, (((1,), (1,)), ((), ())), precision=lax.Precision.HIGHEST)

def product(first, second):
    return jnp.dot(first, second, precision=lax.Precision.HIGHEST)

def reference(points, rhs, basis, transfer, noise, inv_scale, links, leaf_skel, group_skel):
    leaf_pts = points.reshape(DIM, LEAVES, PTS).transpose(1, 0, 2)
    skel_pts = jnp.take_along_axis(leaf_pts, leaf_skel[:, None, :], axis=2)
    group_pts = skel_pts.reshape(GROUPS, BOXES, DIM, SKEL).transpose(0, 2, 1, 3).reshape(GROUPS, DIM, BOXES * SKEL)
    top_pts = jnp.take_along_axis(group_pts, group_skel[:, None, :], axis=2)
    top_all = top_pts.transpose(1, 0, 2).reshape(DIM, GROUPS * SKEL)
    leaf_basis = basis.reshape(LEAVES, PTS, SKEL)
    leaf_noise = noise.reshape(LEAVES, PTS)
    bits = links.astype(jnp.float32)

    def apply(vec):
        leaf_vec = vec.reshape(RHS, LEAVES, PTS).transpose(1, 0, 2)
        coeff = jnp.einsum('lrm,lms->lrs', leaf_vec, leaf_basis, precision=lax.Precision.HIGHEST)
        lifted = jnp.einsum('lrs,lst->lrt', coeff, transfer, precision=lax.Precision.HIGHEST)
        group_coeff = lifted.reshape(GROUPS, BOXES, RHS, SKEL).sum(axis=1)
        top_coeff = group_coeff.transpose(1, 0, 2).reshape(RHS, GROUPS * SKEL)
        box_coeff = coeff.reshape(GROUPS, BOXES, RHS, SKEL).transpose(0, 2, 1, 3).reshape(GROUPS, RHS, BOXES * SKEL)

        def one_leaf(index):
            group = index // BOXES
            lower = jnp.maximum(index - 1, 0)
            upper = jnp.minimum(index + 1, LEAVES - 1)
            own = leaf_pts[index]
            far = contract(box_coeff[group], kernel_block(skel_pts[index], group_pts[group], inv_scale))
            top = contract(top_coeff, kernel_block(top_pts[group], top_all, inv_scale))
            row = far + contract(top, transfer[index])
            total = contract(row, leaf_basis[index])
            left_bit = bits[index, 0]
            right_bit = bits[index, 1]
            near = (1.0 + left_bit + right_bit) * product(leaf_vec[index], kernel_block(own, own, inv_scale))
            near = near + left_bit * product(leaf_vec[lower], kernel_block(leaf_pts[lower], own, inv_scale))
            near = near + right_bit * product(leaf_vec[upper], kernel_block(leaf_pts[upper], own, inv_scale))
            return leaf_noise[index][None, :] * leaf_vec[index] + near + total
        result = lax.map(one_leaf, jnp.arange(LEAVES, dtype=jnp.int32))
        return result.transpose(1, 0, 2).reshape(RHS, NPTS)
    solution = jnp.zeros_like(rhs)
    residual = rhs
    direction = rhs
    norm_now = lax.optimization_barrier(jnp.sum(residual * residual, axis=1))
    for step in range(ITERS):
        image = apply(direction)
        alpha = norm_now / lax.optimization_barrier(jnp.sum(direction * image, axis=1))
        solution = solution + alpha[:, None] * direction
        residual = residual - alpha[:, None] * image
        if step + 1 < ITERS:
            norm_next = lax.optimization_barrier(jnp.sum(residual * residual, axis=1))
            direction = residual + (norm_next / norm_now)[:, None] * direction
            norm_now = norm_next
    return (solution, residual)
```

```python
import functools
import math

import jax
import jax.numpy as jnp
from jax import lax
from jax.experimental import pallas as pl
from jax.experimental.pallas import tpu as pltpu
from jax.sharding import Mesh
from jax.sharding import PartitionSpec as P

GRP_LEAF = ("grp", "leaf_0", "leaf_1", "leaf_2")
MESH = pl.DeviceIdType.MESH
F32 = jnp.float32
BF16 = jnp.bfloat16
FEATURES = 64
LN2 = math.log(2.0)
STRETCH = math.sqrt(5.0) / LN2


def row_of(shape):
    return lax.broadcasted_iota(jnp.int32, shape, 0)


def lane_of(shape):
    return lax.broadcasted_iota(jnp.int32, shape, 1)


def two_parts(value):
    high = value.astype(BF16)
    return high, (value - high.astype(F32)).astype(BF16)


def three_parts(value):
    first = value.astype(BF16).astype(F32)
    rest = value - first
    second = rest.astype(BF16).astype(F32)
    return first, second, (rest - second).astype(BF16).astype(F32)


def features(points, left):
    high, mid, low = three_parts(points)
    norm = jnp.sum(points * points, axis=0, keepdims=True)
    n_high, n_mid, n_low = three_parts(norm)
    row = row_of(points.shape)
    base = 0 if left else 3
    ones = (row >= 3) & (row < 6) if left else row < 3
    norms = jnp.where(
        row == base,
        n_high,
        jnp.where(
            row == base + 1, n_mid, jnp.where(row == base + 2, n_low, jnp.where(ones, 1.0, 0.0))
        ),
    )
    if left:
        two_high, two_mid, two_low = -2.0 * high, -2.0 * mid, -2.0 * low
        pieces = [two_high, two_high, two_mid, two_mid, two_high, two_low]
    else:
        pieces = [high, mid, high, mid, low, high]
    return jnp.concatenate(pieces + [norms, jnp.zeros_like(norms)], axis=0)


def kernel_values(left, right):
    dist = jnp.maximum(jnp.dot(left, right, preferred_element_type=F32), 1e-30)
    scaled = dist * lax.rsqrt(dist)
    return (1.0 + scaled * (LN2 + scaled * (LN2 * LN2 / 3.0))) * jnp.exp2(-scaled)


def fill_block(left_ref, right_ref, high_ref, low_ref):
    rows, columns = high_ref.shape
    tall, wide = min(64, rows), min(256, columns)

    def one(index, carry):
        at = pl.ds(pl.multiple_of(index * tall, tall), tall)
        left = left_ref[at, :]
        for start in range(0, columns, wide):
            values = kernel_values(left, right_ref[:, start : start + wide])
            high, low = two_parts(values)
            high_ref[at, start : start + wide] = high
            low_ref[at, start : start + wide] = low
        return carry

    lax.fori_loop(0, rows // tall, one, 0)


def times(first, second, turned=False):
    dims = (((1,), (1 if turned else 0,)), ((), ()))
    return lax.dot_general(first, second, dims, preferred_element_type=F32)


def product(vec, high, low, turned=False):
    vec_high, vec_low = two_parts(vec)
    rows = vec.shape[0]
    both = times(jnp.concatenate([vec_high, vec_low], axis=0), high, turned)
    return both[:rows] + (both[rows:] + times(vec_high, low, turned))


def side_by_side(buffer, count, start, stop):
    return jnp.concatenate([buffer[slot, start:stop, :] for slot in range(count)], axis=1)


def added_up(buffer, count, start, stop):
    total = buffer[0, start:stop, :]
    for slot in range(1, count):
        total = total + buffer[slot, start:stop, :]
    return total


def lane_sum(value):
    width = value.shape[1]
    total = value[:, :128]
    for start in range(128, width, 128):
        total = total + value[:, start : start + 128]
    return jnp.sum(total, axis=1, keepdims=True)


def everything(
    sizes,
    points_ref,
    rhs_ref,
    basis_ref,
    lift_ref,
    noise_ref,
    leaf_skel_ref,
    group_skel_ref,
    scale_ref,
    links_ref,
    solution_ref,
    residual_ref,
    left_ref,
    right_ref,
    self_high,
    self_low,
    link_high,
    link_low,
    far_high,
    far_low,
    top_high,
    top_low,
    basis_high,
    basis_low,
    lift_high,
    lift_low,
    image_ref,
    points_up,
    vec_up,
    product_out,
    product_in,
    line_1,
    cross_1,
    line_2,
    cross_2_out,
    cross_2_in,
    top_3,
    line_1b,
    cross_1b,
    line_2b,
    cross_2b_out,
    cross_2b_in,
    top_3b,
    sums_1,
    sums_2,
    sums_3,
    send_sem,
    recv_sem,
):
    groups, n_x, n_y, n_core = sizes
    n_cross = n_x * n_core
    boxes = n_cross * n_y
    grp, pos_x, pos_y, pos_core = (lax.axis_index(name) for name in GRP_LEAF)
    box = (pos_x * n_y + pos_y) * n_core + pos_core
    cross = pos_x * n_core + pos_core

    def along_line(step):
        return (grp, pos_x, lax.rem(pos_y + step + n_y, n_y), pos_core)

    def along_cross(step):
        other = lax.rem(cross + step + n_cross, n_cross)
        return (grp, other // n_core, pos_y, lax.rem(other, n_core))

    def along_groups(step):
        return (lax.rem(grp + step + groups, groups), pos_x, pos_y, pos_core)

    def along_boxes(step):
        other = lax.rem(box + step + boxes, boxes)
        return (
            grp,
            other // (n_y * n_core),
            lax.rem(other // n_core, n_y),
            lax.rem(other, n_core),
        )

    barrier = pltpu.get_barrier_semaphore()
    partners = [along_line(step) for step in range(1, n_y)]
    partners += [along_cross(step) for step in range(1, n_cross)]
    partners += [along_groups(step) for step in range(1, groups)]
    partners += [along_boxes(-1), along_boxes(1)]
    for partner in partners:
        pl.semaphore_signal(barrier, inc=1, device_id=partner, device_id_type=MESH)

    started = []

    def send(source, target, device):
        index = len(started)
        copy = pltpu.make_async_remote_copy(
            src_ref=source,
            dst_ref=target,
            send_sem=send_sem.at[index],
            recv_sem=recv_sem.at[index],
            device_id=device,
            device_id_type=MESH,
        )
        copy.start()
        started.append(copy)
        return copy

    def spread(buffer, count, along):
        order = sorted(range(1, count), key=lambda step: -min(step, count - step))
        return [send(buffer.at[0], buffer.at[step], along(step)) for step in order]

    def arrived(copies):
        for copy in copies:
            copy.wait_recv()

    inv_column = jnp.zeros((8, 1), F32)
    for dim in range(8):
        inv_column = jnp.where(row_of((8, 1)) == dim, scale_ref[dim], inv_column)
    inv_column = inv_column * STRETCH
    left_bit = links_ref[0, 0].astype(F32)
    right_bit = links_ref[0, 1].astype(F32)
    weight_self = 1.0 + left_bit + right_bit

    basis_high[...], basis_low[...] = two_parts(basis_ref[...])
    lift_high[...], lift_low[...] = two_parts(lift_ref[0])
    rhs = rhs_ref[...]
    coeff = product(rhs, basis_high[...], basis_low[...])
    lifted = product(coeff, lift_high[...], lift_low[...])
    own = points_ref[...] * inv_column
    width = own.shape[1]
    picked = jnp.where(row_of((width, 128)) == leaf_skel_ref[...], 1.0, 0.0).astype(BF16)
    parts = times(jnp.concatenate(three_parts(own), axis=0).astype(BF16), picked)
    skel = parts[:8] + (parts[8:16] + parts[16:])
    held = jnp.where(row_of((128, 128)) == group_skel_ref[...] - box * 128, 1.0, 0.0).astype(BF16)
    parts = times(jnp.concatenate(three_parts(skel), axis=0).astype(BF16), held)
    top_part = parts[:8] + (parts[8:16] + parts[16:])
    line_1[0, :16, :] = coeff
    line_1[0, 16:, :] = skel
    cross_1[0, :16, :] = lifted
    cross_1[0, 16:24, :] = skel
    cross_1[0, 24:, :] = top_part

    pl.semaphore_wait(barrier, len(partners))
    cross_1_copies = spread(cross_1, n_cross, along_cross)
    line_1_copies = spread(line_1, n_y, along_line)
    points_copy = send(points_ref, points_up, along_boxes(-1))
    vec_copy = send(rhs_ref, vec_up.at[0], along_boxes(-1))

    left_ref[...] = features(own, True).T.astype(BF16)
    right_ref[...] = features(own, False).astype(BF16)
    fill_block(left_ref, right_ref, self_high, self_low)

    arrived(cross_1_copies)
    line_2[0, :16, :] = added_up(cross_1, n_cross, 0, 16)
    line_2[0, 16:, :] = added_up(cross_1, n_cross, 24, 32)
    line_2_copies = spread(line_2, n_y, along_line)

    arrived([points_copy, vec_copy])
    right_ref[...] = features(points_up[...] * inv_column, False).astype(BF16)
    fill_block(left_ref, right_ref, link_high, link_low)
    product_out[0] = right_bit * product(rhs, link_high[...], link_low[...])
    product_copy = send(product_out.at[0], product_in.at[0], along_boxes(1))

    arrived(line_1_copies)
    far_left = features(side_by_side(line_1, n_y, 16, 24), True).T
    left_ref[: n_y * 128, :] = far_left.astype(BF16)
    far_right = features(side_by_side(cross_1, n_cross, 16, 24), False)
    right_ref[:, : n_cross * 128] = far_right.astype(BF16)
    fill_block(left_ref, right_ref, far_high, far_low)

    arrived(line_2_copies)
    top_3[0, :16, :] = added_up(line_2, n_y, 0, 16)
    top_own = added_up(line_2, n_y, 16, 24)
    top_3[0, 16:, :] = top_own
    top_3_copies = spread(top_3, groups, along_groups)

    def far_terms(coeffs, out, into):
        spread_out = product(coeffs, far_high[...], far_low[...])
        out[0] = spread_out[:, :128]
        copies = []
        for slot in range(1, n_cross):
            out[slot] = spread_out[:, slot * 128 : (slot + 1) * 128]
        order = sorted(range(1, n_cross), key=lambda step: -min(step, n_cross - step))
        for slot in order:
            copies.append(send(out.at[slot], into.at[slot], along_cross(-slot)))
        return copies

    def far_sum(out, into):
        total = out[0]
        for slot in range(1, n_cross):
            total = total + into[slot]
        return total

    cross_2_copies = far_terms(side_by_side(line_1, n_y, 0, 16), cross_2_out, cross_2_in)

    noise = noise_ref[...]

    def near_part(vec, above):
        return (
            noise * vec
            + weight_self * product(vec, self_high[...], self_low[...])
            + right_bit * product(above, link_high[...], link_low[...], True)
        )

    def rest(far, top_coeff):
        top = product(top_coeff, top_high[...], top_low[...])
        row = far + product(top, lift_high[...], lift_low[...], True)
        return product(row, basis_high[...], basis_low[...], True)

    near = near_part(rhs, vec_up[0])
    dot_rr = lane_sum(rhs * rhs)

    arrived(cross_2_copies)
    far = far_sum(cross_2_out, cross_2_in)
    arrived(top_3_copies)
    top_left = features(side_by_side(top_3, groups, 16, 24), True).T
    left_ref[: groups * 128, :] = top_left.astype(BF16)
    right_ref[:, :128] = features(top_own, False).astype(BF16)
    fill_block(left_ref, right_ref.at[:, :128], top_high, top_low)
    image = near + rest(far, side_by_side(top_3, groups, 0, 16))
    arrived([product_copy])
    image = image + product_in[0]
    image_ref[...] = image

    coeff = product(image, basis_high[...], basis_low[...])
    line_1b[0] = coeff
    line_1b_copies = spread(line_1b, n_y, along_line)
    cross_1b[0] = product(coeff, lift_high[...], lift_low[...])
    cross_1b_copies = spread(cross_1b, n_cross, along_cross)
    vec_copy = send(image_ref, vec_up.at[1], along_boxes(-1))
    product_out[1] = right_bit * product(image, link_high[...], link_low[...])
    product_copy = send(product_out.at[1], product_in.at[1], along_boxes(1))
    arrived(cross_1b_copies)
    line_2b[0] = added_up(cross_1b, n_cross, 0, 16)
    line_2b_copies = spread(line_2b, n_y, along_line)
    arrived(line_1b_copies)
    cross_2b_copies = far_terms(side_by_side(line_1b, n_y, 0, 16), cross_2b_out, cross_2b_in)
    arrived([vec_copy])
    near = near_part(image, vec_up[1])
    arrived(line_2b_copies)
    top_3b[0] = added_up(line_2b, n_y, 0, 16)
    top_3b_copies = spread(top_3b, groups, along_groups)
    dot_rw = lane_sum(rhs * image)
    dot_ww = lane_sum(image * image)
    arrived([product_copy])
    near = near + product_in[1]
    arrived(cross_2b_copies)
    far = far_sum(cross_2b_out, cross_2b_in)
    arrived(top_3b_copies)
    second = near + rest(far, side_by_side(top_3b, groups, 0, 16))
    dot_wu = lane_sum(image * second)

    lane = lane_of((8, 128))
    packed = jnp.zeros((8, 128), F32)
    for index, dot in enumerate((dot_rr, dot_rw, dot_ww, dot_wu)):
        packed = jnp.where(lane == index, dot[:8], packed)
        packed = jnp.where(lane == index + 4, dot[8:], packed)
    sums_1[0] = packed
    arrived(spread(sums_1, n_y, along_line))
    sums_2[0] = added_up(sums_1, n_y, 0, 8)
    arrived(spread(sums_2, n_cross, along_cross))
    sums_3[0] = added_up(sums_2, n_cross, 0, 8)
    arrived(spread(sums_3, groups, along_groups))
    total = added_up(sums_3, groups, 0, 8)
    rr, rw, ww, wu = (
        jnp.concatenate([total[:, index : index + 1], total[:, index + 4 : index + 5]], axis=0)
        for index in range(4)
    )

    alpha = rr / rw
    next_rr = rr - 2.0 * alpha * rw + alpha * alpha * ww
    curve = rw - 2.0 * alpha * ww + alpha * alpha * wu
    ratio = next_rr / rr
    next_alpha = next_rr / (curve - ratio * next_rr / alpha)
    one = alpha + next_alpha * (1.0 + ratio)
    two = alpha * next_alpha
    solution_ref[...] = one * rhs - two * image
    residual_ref[...] = rhs - one * image + two * second

    for copy in started:
        copy.wait_send()


def copies_of(sizes):
    groups, n_x, n_y, n_core = sizes
    n_cross = n_x * n_core
    return 5 * (n_y - 1) + 5 * (n_cross - 1) + 3 * (groups - 1) + 5


def local(sizes, points, rhs, basis, transfer, noise, inv_scale, links, leaf_skel, group_skel):
    groups, n_x, n_y, n_core = sizes
    n_cross = n_x * n_core
    width = points.shape[1]
    rows = rhs.shape[0]
    skel = leaf_skel.shape[1]
    vmem = pl.BlockSpec(memory_space=pltpu.VMEM)
    smem = pl.BlockSpec(memory_space=pltpu.SMEM)
    count = copies_of(sizes)

    def held(*shape):
        return pltpu.VMEM(shape, F32)

    def halves(*shape):
        return [pltpu.VMEM(shape, BF16)] * 2

    scratch = [
        pltpu.VMEM((width, FEATURES), BF16),
        pltpu.VMEM((FEATURES, width), BF16),
        *halves(width, width),
        *halves(width, width),
        *halves(n_y * skel, n_cross * skel),
        *halves(groups * skel, skel),
        *halves(width, skel),
        *halves(skel, skel),
        held(rows, width),
        held(8, width),
        held(2, rows, width),
        held(2, rows, width),
        held(2, rows, width),
        held(n_y, rows + 8, skel),
        held(n_cross, rows + 16, skel),
        held(n_y, rows + 8, skel),
        held(n_cross, rows, skel),
        held(n_cross, rows, skel),
        held(groups, rows + 8, skel),
        held(n_y, rows, skel),
        held(n_cross, rows, skel),
        held(n_y, rows, skel),
        held(n_cross, rows, skel),
        held(n_cross, rows, skel),
        held(groups, rows, skel),
        held(n_y, 8, skel),
        held(n_cross, 8, skel),
        held(groups, 8, skel),
        pltpu.SemaphoreType.DMA((count,)),
        pltpu.SemaphoreType.DMA((count,)),
    ]
    return pl.pallas_call(
        functools.partial(everything, sizes),
        name="skeleton_cg",
        out_shape=(jax.ShapeDtypeStruct(rhs.shape, F32), jax.ShapeDtypeStruct(rhs.shape, F32)),
        in_specs=[vmem, vmem, vmem, vmem, vmem, vmem, vmem, smem, smem],
        out_specs=(vmem, vmem),
        scratch_shapes=scratch,
        compiler_params=pltpu.CompilerParams(
            collective_id=0, has_side_effects=True, vmem_limit_bytes=48 * 1024 * 1024
        ),
    )(
        points,
        rhs,
        basis,
        transfer,
        noise[None, :],
        leaf_skel,
        group_skel,
        inv_scale,
        links,
    )


def on_finer(finer):
    placed = (
        P(None, GRP_LEAF),
        P(None, GRP_LEAF),
        P(GRP_LEAF, None),
        P(GRP_LEAF, None, None),
        P(GRP_LEAF),
        P(),
        P(GRP_LEAF, None),
        P(GRP_LEAF, None),
        P("grp", None),
    )
    sizes = tuple(finer.shape[name] for name in GRP_LEAF)
    return jax.shard_map(
        functools.partial(local, sizes),
        mesh=finer,
        in_specs=placed,
        out_specs=(P(None, GRP_LEAF), P(None, GRP_LEAF)),
        check_vma=False,
    )


def solution(mesh):
    finer = Mesh(mesh.devices.reshape(mesh.shape["grp"], 4, 8, 2), GRP_LEAF)
    return on_finer(finer)
```

```python
import functools
import math

import jax
import jax.numpy as jnp
from jax import lax
from jax.experimental import pallas as pl
from jax.experimental.pallas import tpu as pltpu
from jax.sharding import Mesh
from jax.sharding import PartitionSpec as P

GRP_LEAF = ("grp", "leaf_0", "leaf_1", "leaf_2")
MESH = pl.DeviceIdType.MESH
F32 = jnp.float32
BF16 = jnp.bfloat16
FEATURES = 64
LN2 = math.log(2.0)
STRETCH = math.sqrt(5.0) / LN2


def row_of(shape):
    return lax.broadcasted_iota(jnp.int32, shape, 0)


def lane_of(shape):
    return lax.broadcasted_iota(jnp.int32, shape, 1)


def two_parts(value):
    high = value.astype(BF16)
    return high, (value - high.astype(F32)).astype(BF16)


def three_parts(value):
    first = value.astype(BF16).astype(F32)
    rest = value - first
    second = rest.astype(BF16).astype(F32)
    return first, second, (rest - second).astype(BF16).astype(F32)


def features(points, left):
    high, mid, low = three_parts(points)
    norm = jnp.sum(points * points, axis=0, keepdims=True)
    n_high, n_mid, n_low = three_parts(norm)
    row = row_of(points.shape)
    base = 0 if left else 3
    ones = (row >= 3) & (row < 6) if left else row < 3
    norms = jnp.where(
        row == base,
        n_high,
        jnp.where(
            row == base + 1, n_mid, jnp.where(row == base + 2, n_low, jnp.where(ones, 1.0, 0.0))
        ),
    )
    if left:
        two_high, two_mid, two_low = -2.0 * high, -2.0 * mid, -2.0 * low
        pieces = [two_high, two_high, two_mid, two_mid, two_high, two_low]
    else:
        pieces = [high, mid, high, mid, low, high]
    return jnp.concatenate(pieces + [norms, jnp.zeros_like(norms)], axis=0)


def kernel_values(left, right):
    dist = jnp.maximum(jnp.dot(left, right, preferred_element_type=F32), 1e-30)
    scaled = dist * lax.rsqrt(dist)
    return (1.0 + scaled * (LN2 + scaled * (LN2 * LN2 / 3.0))) * jnp.exp2(-scaled)


def fill_block(left_ref, right_ref, high_ref, low_ref, first=0, last=None):
    rows, columns = high_ref.shape
    last = columns if last is None else last
    wide = min(256, last - first)
    tall = min(rows, 64 if last - first > 256 else 256)

    def one(index, carry):
        at = pl.ds(pl.multiple_of(index * tall, tall), tall)
        left = left_ref[at, :]
        for start in range(first, last, wide):
            stop = min(start + wide, last)
            values = kernel_values(left, right_ref[:, start:stop])
            high, low = two_parts(values)
            high_ref[at, start:stop] = high
            low_ref[at, start:stop] = low
        return carry

    lax.fori_loop(0, rows // tall, one, 0)


def times(first, second, turned=False):
    dims = (((1,), (1 if turned else 0,)), ((), ()))
    return lax.dot_general(first, second, dims, preferred_element_type=F32)


def product(vec, high, low, turned=False):
    vec_high, vec_low = two_parts(vec)
    rows = vec.shape[0]
    both = times(jnp.concatenate([vec_high, vec_low], axis=0), high, turned)
    return both[:rows] + (both[rows:] + times(vec_high, low, turned))


def side_by_side(buffer, count, start, stop):
    return jnp.concatenate([buffer[slot, start:stop, :] for slot in range(count)], axis=1)


def added_up(buffer, count, start, stop):
    total = buffer[0, start:stop, :]
    for slot in range(1, count):
        total = total + buffer[slot, start:stop, :]
    return total


def lane_sum(value):
    width = value.shape[1]
    total = value[:, :128]
    for start in range(128, width, 128):
        total = total + value[:, start : start + 128]
    return jnp.sum(total, axis=1, keepdims=True)


def everything(
    sizes,
    points_hbm,
    rhs_hbm,
    basis_hbm,
    lift_hbm,
    noise_hbm,
    scale_hbm,
    links_hbm,
    leaf_skel_hbm,
    group_skel_hbm,
    image_ref,
    second_ref,
    one_ref,
    two_ref,
    points_ref,
    rhs_ref,
    basis_ref,
    lift_ref,
    noise_ref,
    scale_ref,
    links_ref,
    leaf_skel_ref,
    group_skel_ref,
    left_ref,
    right_ref,
    top_left_ref,
    top_right_ref,
    self_high,
    self_low,
    link_high,
    link_low,
    far_high,
    far_low,
    top_high,
    top_low,
    basis_high,
    basis_low,
    turned_high,
    turned_low,
    lift_high,
    lift_low,
    lower_high,
    lower_low,
    gram_high,
    gram_low,
    jump_high,
    jump_low,
    points_up,
    vec_up,
    product_out,
    product_in,
    line_1,
    cross_1,
    line_2,
    cross_2_out,
    cross_2_in,
    top_3,
    line_1b,
    cross_1b,
    line_2b,
    cross_2b_out,
    cross_2b_in,
    top_3b,
    sums_1,
    sums_2,
    sums_3,
    load_sem,
    send_sem,
    recv_sem,
):
    groups, n_x, n_y, n_core = sizes
    n_cross = n_x * n_core
    boxes = n_cross * n_y
    grp, pos_x, pos_y, pos_core = (lax.axis_index(name) for name in GRP_LEAF)
    box = (pos_x * n_y + pos_y) * n_core + pos_core
    cross = pos_x * n_core + pos_core

    def along_line(step):
        return (grp, pos_x, lax.rem(pos_y + step + n_y, n_y), pos_core)

    def along_cross(step):
        other = lax.rem(cross + step + n_cross, n_cross)
        return (grp, other // n_core, pos_y, lax.rem(other, n_core))

    def along_groups(step):
        return (lax.rem(grp + step + groups, groups), pos_x, pos_y, pos_core)

    def along_boxes(step):
        other = lax.rem(box + step + boxes, boxes)
        return (
            grp,
            other // (n_y * n_core),
            lax.rem(other // n_core, n_y),
            lax.rem(other, n_core),
        )

    loads = {}
    for index, (name, source, target) in enumerate(
        (
            ("rhs", rhs_hbm, rhs_ref),
            ("basis", basis_hbm, basis_ref),
            ("lift", lift_hbm, lift_ref),
            ("points", points_hbm, points_ref),
            ("scale", scale_hbm, scale_ref),
            ("leaf_skel", leaf_skel_hbm, leaf_skel_ref),
            ("group_skel", group_skel_hbm, group_skel_ref),
            ("links", links_hbm, links_ref),
            ("noise", noise_hbm, noise_ref),
        )
    ):
        loads[name] = pltpu.make_async_copy(source, target, load_sem.at[index])
        loads[name].start()

    barrier = pltpu.get_barrier_semaphore()
    partners = [along_groups(step) for step in range(1, groups)]
    partners += [along_line(step) for step in range(1, n_y)]
    partners += [along_cross(step) for step in range(1, n_cross)]
    partners += [along_boxes(-1), along_boxes(1)]
    for partner in partners:
        pl.semaphore_signal(barrier, inc=1, device_id=partner, device_id_type=MESH)

    started = []

    def send(source, target, device):
        index = len(started)
        copy = pltpu.make_async_remote_copy(
            src_ref=source,
            dst_ref=target,
            send_sem=send_sem.at[index],
            recv_sem=recv_sem.at[index],
            device_id=device,
            device_id_type=MESH,
        )
        copy.start()
        started.append(copy)
        return copy

    def spread(buffer, count, along):
        order = sorted(range(1, count), key=lambda step: -min(step, count - step))
        return [send(buffer.at[0], buffer.at[step], along(step)) for step in order]

    def arrived(copies):
        for copy in copies:
            copy.wait_recv()

    def keep(value, high_ref, low_ref):
        high_ref[...], low_ref[...] = two_parts(value)

    loads["rhs"].wait()
    loads["basis"].wait()
    rhs = rhs_ref[...]
    keep(basis_ref[...], basis_high, basis_low)
    coeff = product(rhs, basis_high[...], basis_low[...])
    loads["lift"].wait()
    keep(lift_ref[0], lift_high, lift_low)
    lifted = product(coeff, lift_high[...], lift_low[...])
    loads["points"].wait()
    loads["scale"].wait()
    loads["leaf_skel"].wait()
    loads["group_skel"].wait()
    diagonal = row_of((8, 8)) == lane_of((8, 8))
    inv_column = jnp.sum(jnp.where(diagonal, scale_ref[...], 0.0), axis=1, keepdims=True) * STRETCH
    own = points_ref[...] * inv_column
    width = own.shape[1]
    picked = jnp.where(row_of((width, 128)) == leaf_skel_ref[...], 1.0, 0.0).astype(BF16)
    parts = times(jnp.concatenate(three_parts(own), axis=0).astype(BF16), picked)
    skel = parts[:8] + (parts[8:16] + parts[16:])
    held = jnp.where(row_of((128, 128)) == group_skel_ref[...] - box * 128, 1.0, 0.0).astype(BF16)
    parts = times(jnp.concatenate(three_parts(skel), axis=0).astype(BF16), held)
    top_part = parts[:8] + (parts[8:16] + parts[16:])
    cross_1[0, :16, :] = lifted
    cross_1[0, 16:24, :] = skel
    cross_1[0, 24:, :] = top_part
    line_1[0, :16, :] = coeff
    line_1[0, 16:, :] = skel

    pl.semaphore_wait(barrier, len(partners))
    cross_1_copies = spread(cross_1, n_cross, along_cross)
    line_1_copies = spread(line_1, n_y, along_line)
    points_copy = send(points_ref, points_up, along_boxes(-1))
    vec_copy = send(rhs_ref, vec_up.at[0], along_boxes(-1))

    loads["links"].wait()
    loads["noise"].wait()
    right_bit = links_ref[:, 1:2].astype(F32)
    weight_self = 1.0 + links_ref[:, 0:1].astype(F32) + right_bit
    left_ref[...] = features(own, True).T.astype(BF16)
    right_ref[...] = features(own, False).astype(BF16)
    fill_block(left_ref, right_ref, self_high, self_low)

    arrived(cross_1_copies)
    line_2[0, :16, :] = added_up(cross_1, n_cross, 0, 16)
    line_2[0, 16:, :] = added_up(cross_1, n_cross, 24, 32)
    line_2_copies = spread(line_2, n_y, along_line)

    arrived([points_copy, vec_copy])
    right_ref[...] = features(points_up[...] * inv_column, False).astype(BF16)
    fill_block(left_ref, right_ref, link_high, link_low)
    product_out[0] = right_bit * product(rhs, link_high[...], link_low[...])
    product_copy = send(product_out.at[0], product_in.at[0], along_boxes(1))

    arrived(line_1_copies)
    far_left = features(side_by_side(line_1, n_y, 16, 24), True).T
    left_ref[: n_y * 128, :] = far_left.astype(BF16)
    far_right = features(side_by_side(cross_1, n_cross, 16, 24), False)
    right_ref[:, : n_cross * 128] = far_right.astype(BF16)
    fill_block(left_ref, right_ref, far_high, far_low)

    arrived(line_2_copies)
    top_3[0, :16, :] = added_up(line_2, n_y, 0, 16)
    top_own = added_up(line_2, n_y, 16, 24)
    top_3[0, 16:, :] = top_own
    top_3_copies = spread(top_3, groups, along_groups)

    def far_terms(spread_out, out, into):
        for slot in range(n_cross):
            out[slot] = spread_out[:, slot * 128 : (slot + 1) * 128]
        order = sorted(range(1, n_cross), key=lambda step: -min(step, n_cross - step))
        return [send(out.at[slot], into.at[slot], along_cross(-slot)) for slot in order]

    def far_sum(out, into):
        total = out[0]
        for slot in range(1, n_cross):
            total = total + into[slot]
        return total

    line_coeff = side_by_side(line_1, n_y, 0, 16)
    cross_2_copies = far_terms(
        product(line_coeff, far_high[...], far_low[...]), cross_2_out, cross_2_in
    )

    noise = noise_ref[...]

    def self_part(vec):
        return noise * vec + weight_self * product(vec, self_high[...], self_low[...])

    def upper_part(above):
        return right_bit * product(above, link_high[...], link_low[...], True)

    near = self_part(rhs) + upper_part(vec_up[0])

    turned = basis_ref[...].T
    keep(turned, turned_high, turned_low)
    gram = product(turned, basis_high[...], basis_low[...])
    both = jnp.concatenate([gram, product(gram, lift_high[...], lift_low[...])], axis=1)
    keep(both, gram_high, gram_low)
    lower = lift_ref[0].T
    keep(lower, lower_high, lower_low)
    keep(product(lower, gram_high[...], gram_low[...]), jump_high, jump_low)
    dot_rr = lane_sum(rhs * rhs)

    arrived([product_copy])
    near = near + product_in[0]
    image_ref[...] = near
    near_coeff = product(near, basis_high[...], basis_low[...])
    known = jnp.concatenate(
        [near_coeff, product(near_coeff, lift_high[...], lift_low[...])], axis=1
    )
    arrived(cross_2_copies)
    far = far_sum(cross_2_out, cross_2_in)
    known = known + product(far, gram_high[...], gram_low[...])
    top_right_ref[:, :128] = features(top_own, False).astype(BF16)

    arrived(top_3_copies)
    top_all = side_by_side(top_3, groups, 16, 24)
    top_left_ref[...] = features(top_all, True).T.astype(BF16)
    fill_block(top_left_ref, top_right_ref, top_high, top_low, 0, 128)
    top = product(side_by_side(top_3, groups, 0, 16), top_high[:, :128], top_low[:, :128])
    both = known + product(top, jump_high[...], jump_low[...])
    coeff = both[:, :128]
    cross_1b[0, :16, :] = both[:, 128:]
    cross_1b[0, 16:, :] = coeff
    line_1b[0] = coeff
    line_1b_copies = spread(line_1b, n_y, along_line)
    cross_1b_copies = spread(cross_1b, n_cross, along_cross)
    row = far + product(top, lower_high[...], lower_low[...])
    image = image_ref[...] + product(row, turned_high[...], turned_low[...])
    image_ref[...] = image
    vec_copy = send(image_ref, vec_up.at[1], along_boxes(-1))
    product_out[1] = right_bit * product(image, link_high[...], link_low[...])
    product_copy = send(product_out.at[1], product_in.at[1], along_boxes(1))
    near = self_part(image)
    dot_rw = lane_sum(rhs * image)
    dot_ww = lane_sum(image * image)
    dot_wu = lane_sum(image * near)
    arrived(cross_1b_copies)
    line_2b[0] = added_up(cross_1b, n_cross, 0, 16)
    line_2b_copies = spread(line_2b, n_y, along_line)
    arrived([vec_copy])
    upper = upper_part(vec_up[1])
    dot_wu = dot_wu + 2.0 * lane_sum(image * upper)
    second_ref[...] = near + upper
    arrived(line_1b_copies)
    spread_out = product(side_by_side(line_1b, n_y, 0, 16), far_high[...], far_low[...])
    cross_2b_copies = far_terms(spread_out, cross_2b_out, cross_2b_in)
    dot_wu = dot_wu + lane_sum(spread_out * side_by_side(cross_1b, n_cross, 16, 32))

    lane = lane_of((8, 128))
    packed = jnp.zeros((8, 128), F32)
    for index, dot in enumerate((dot_rr, dot_rw, dot_ww, dot_wu)):
        packed = jnp.where(lane == index, dot[:8], packed)
        packed = jnp.where(lane == index + 4, dot[8:], packed)
    sums_1[0] = packed
    sums_1_copies = spread(sums_1, n_cross, along_cross)

    top_right_ref[...] = features(top_all, False).astype(BF16)
    fill_block(top_left_ref, top_right_ref, top_high, top_low, 128)

    arrived(line_2b_copies)
    top_3b[0] = added_up(line_2b, n_y, 0, 16)
    top_3b_copies = spread(top_3b, groups, along_groups)
    arrived(sums_1_copies)
    sums_2[0] = added_up(sums_1, n_cross, 0, 8)
    sums_2_copies = spread(sums_2, n_y, along_line)
    arrived([product_copy])
    arrived(cross_2b_copies)
    far = far_sum(cross_2b_out, cross_2b_in)
    arrived(sums_2_copies)
    sums_3[0] = added_up(sums_2, n_y, 0, 8)
    sums_3_copies = spread(sums_3, groups, along_groups)
    arrived(top_3b_copies)
    top_coeff = side_by_side(top_3b, groups, 0, 16)
    top_out = product(top_coeff, top_high[...], top_low[...])
    row = far + product(top_out[:, :128], lower_high[...], lower_low[...])
    second_ref[...] = (
        second_ref[...] + product_in[1] + product(row, turned_high[...], turned_low[...])
    )
    top_wu = lane_sum(top_out * top_coeff)
    arrived(sums_3_copies)
    total = added_up(sums_3, groups, 0, 8)
    rr, rw, ww, wu = (
        jnp.concatenate([total[:, index : index + 1], total[:, index + 4 : index + 5]], axis=0)
        for index in range(4)
    )
    wu = wu + top_wu

    alpha = rr / rw
    next_rr = rr - 2.0 * alpha * rw + alpha * alpha * ww
    curve = rw - 2.0 * alpha * ww + alpha * alpha * wu
    ratio = next_rr / rr
    next_alpha = next_rr / (curve - ratio * next_rr / alpha)
    one_ref[...] = jnp.broadcast_to(alpha + next_alpha * (1.0 + ratio), one_ref.shape)
    two_ref[...] = jnp.broadcast_to(alpha * next_alpha, two_ref.shape)

    for copy in started:
        copy.wait_send()


def copies_of(sizes):
    groups, n_x, n_y, n_core = sizes
    n_cross = n_x * n_core
    return 5 * (n_y - 1) + 5 * (n_cross - 1) + 3 * (groups - 1) + 5


def local(sizes, points, rhs, basis, transfer, noise, inv_scale, links, leaf_skel, group_skel):
    groups, n_x, n_y, n_core = sizes
    n_cross = n_x * n_core
    width = points.shape[1]
    rows = rhs.shape[0]
    skel = leaf_skel.shape[1]
    count = copies_of(sizes)
    operands = (
        points,
        rhs,
        basis,
        transfer,
        noise[None, :],
        inv_scale[None, :],
        links,
        leaf_skel,
        group_skel,
    )

    def held(*shape):
        return pltpu.VMEM(shape, F32)

    def halves(*shape):
        return [pltpu.VMEM(shape, BF16)] * 2

    scratch = [
        *[pltpu.VMEM(operand.shape, operand.dtype) for operand in operands],
        pltpu.VMEM((width, FEATURES), BF16),
        pltpu.VMEM((FEATURES, width), BF16),
        pltpu.VMEM((groups * skel, FEATURES), BF16),
        pltpu.VMEM((FEATURES, groups * skel), BF16),
        *halves(width, width),
        *halves(width, width),
        *halves(n_y * skel, n_cross * skel),
        *halves(groups * skel, groups * skel),
        *halves(width, skel),
        *halves(skel, width),
        *halves(skel, skel),
        *halves(skel, skel),
        *halves(skel, 2 * skel),
        *halves(skel, 2 * skel),
        held(8, width),
        held(2, rows, width),
        held(2, rows, width),
        held(2, rows, width),
        held(n_y, rows + 8, skel),
        held(n_cross, rows + 16, skel),
        held(n_y, rows + 8, skel),
        held(n_cross, rows, skel),
        held(n_cross, rows, skel),
        held(groups, rows + 8, skel),
        held(n_y, rows, skel),
        held(n_cross, 2 * rows, skel),
        held(n_y, rows, skel),
        held(n_cross, rows, skel),
        held(n_cross, rows, skel),
        held(groups, rows, skel),
        held(n_cross, 8, skel),
        held(n_y, 8, skel),
        held(groups, 8, skel),
        pltpu.SemaphoreType.DMA((len(operands),)),
        pltpu.SemaphoreType.DMA((count,)),
        pltpu.SemaphoreType.DMA((count,)),
    ]
    vmem = pl.BlockSpec(memory_space=pltpu.VMEM)
    image, second, one, two = pl.pallas_call(
        functools.partial(everything, sizes),
        name="skeleton_cg",
        out_shape=[jax.ShapeDtypeStruct(rhs.shape, F32)] * 4,
        in_specs=[pl.BlockSpec(memory_space=pltpu.HBM)] * len(operands),
        out_specs=[vmem] * 4,
        scratch_shapes=scratch,
        compiler_params=pltpu.CompilerParams(
            collective_id=0, has_side_effects=True
        ),
    )(*operands)
    return one * rhs - two * image, rhs - one * image + two * second


def on_finer(finer):
    placed = (
        P(None, GRP_LEAF),
        P(None, GRP_LEAF),
        P(GRP_LEAF, None),
        P(GRP_LEAF, None, None),
        P(GRP_LEAF),
        P(),
        P(GRP_LEAF, None),
        P(GRP_LEAF, None),
        P("grp", None),
    )
    sizes = tuple(finer.shape[name] for name in GRP_LEAF)
    return jax.shard_map(
        functools.partial(local, sizes),
        mesh=finer,
        in_specs=placed,
        out_specs=(P(None, GRP_LEAF), P(None, GRP_LEAF)),
        check_vma=False,
    )


def solution(mesh):
    finer = Mesh(mesh.devices.reshape(mesh.shape["grp"], 4, 8, 2), GRP_LEAF)
    return on_finer(finer)
```

```python
import functools
import math

import jax
import jax.numpy as jnp
from jax import lax
from jax.experimental import pallas as pl
from jax.experimental.pallas import tpu as pltpu
from jax.sharding import Mesh
from jax.sharding import PartitionSpec as P

GRP_LEAF = ("grp", "leaf_0", "leaf_1", "leaf_2")
MESH = pl.DeviceIdType.MESH
F32 = jnp.float32
BF16 = jnp.bfloat16
FEATURES = 64
LN2 = math.log(2.0)
STRETCH = math.sqrt(5.0) / LN2


def row_of(shape):
    return lax.broadcasted_iota(jnp.int32, shape, 0)


def lane_of(shape):
    return lax.broadcasted_iota(jnp.int32, shape, 1)


def two_parts(value):
    high = value.astype(BF16)
    return high, (value - high.astype(F32)).astype(BF16)


def three_parts(value):
    first = value.astype(BF16).astype(F32)
    rest = value - first
    second = rest.astype(BF16).astype(F32)
    return first, second, (rest - second).astype(BF16).astype(F32)


def features(points, left):
    high, mid, low = three_parts(points)
    norm = jnp.sum(points * points, axis=0, keepdims=True)
    n_high, n_mid, n_low = three_parts(norm)
    row = row_of(points.shape)
    base = 0 if left else 3
    ones = (row >= 3) & (row < 6) if left else row < 3
    norms = jnp.where(
        row == base,
        n_high,
        jnp.where(
            row == base + 1, n_mid, jnp.where(row == base + 2, n_low, jnp.where(ones, 1.0, 0.0))
        ),
    )
    if left:
        two_high, two_mid, two_low = -2.0 * high, -2.0 * mid, -2.0 * low
        pieces = [two_high, two_high, two_mid, two_mid, two_high, two_low]
    else:
        pieces = [high, mid, high, mid, low, high]
    return jnp.concatenate(pieces + [norms, jnp.zeros_like(norms)], axis=0)


def kernel_values(left, right):
    dist = jnp.maximum(jnp.dot(left, right, preferred_element_type=F32), 1e-30)
    scaled = dist * lax.rsqrt(dist)
    return (1.0 + scaled * (LN2 + scaled * (LN2 * LN2 / 3.0))) * jnp.exp2(-scaled)


def fill_block(left_ref, right_ref, high_ref, low_ref, first=0, last=None, top=0, bottom=None):
    last = high_ref.shape[1] if last is None else last
    bottom = high_ref.shape[0] if bottom is None else bottom
    wide = min(256, last - first)
    tall = min(bottom - top, 1024 if last - first <= 128 else 512)

    def one(index, carry):
        at = pl.ds(pl.multiple_of(top + index * tall, tall), tall)
        left = left_ref[at, :]
        for start in range(first, last, wide):
            stop = min(start + wide, last)
            values = kernel_values(left, right_ref[:, start:stop])
            high, low = two_parts(values)
            high_ref[at, start:stop] = high
            low_ref[at, start:stop] = low
        return carry

    lax.fori_loop(0, (bottom - top) // tall, one, 0)


def times(first, second, turned=False):
    dims = (((1,), (1 if turned else 0,)), ((), ()))
    return lax.dot_general(first, second, dims, preferred_element_type=F32)


def product(vec, high, low, turned=False):
    vec_high, vec_low = two_parts(vec)
    rows = vec.shape[0]
    both = times(jnp.concatenate([vec_high, vec_low], axis=0), high, turned)
    return both[:rows] + (both[rows:] + times(vec_high, low, turned))


def side_by_side(buffer, count, start, stop):
    return jnp.concatenate([buffer[slot, start:stop, :] for slot in range(count)], axis=1)


def added_up(buffer, count, start, stop):
    total = buffer[0, start:stop, :]
    for slot in range(1, count):
        total = total + buffer[slot, start:stop, :]
    return total


def lane_sum(value):
    width = value.shape[1]
    total = value[:, :128]
    for start in range(128, width, 128):
        total = total + value[:, start : start + 128]
    return jnp.sum(total, axis=1, keepdims=True)


def everything(
    sizes,
    points_hbm,
    rhs_hbm,
    basis_hbm,
    lift_hbm,
    noise_hbm,
    scale_hbm,
    links_hbm,
    leaf_skel_hbm,
    group_skel_hbm,
    image_ref,
    second_ref,
    one_ref,
    two_ref,
    points_ref,
    rhs_ref,
    basis_ref,
    lift_ref,
    noise_ref,
    scale_ref,
    links_ref,
    leaf_skel_ref,
    group_skel_ref,
    left_ref,
    right_ref,
    top_left_ref,
    top_right_ref,
    self_high,
    self_low,
    link_high,
    link_low,
    far_high,
    far_low,
    top_high,
    top_low,
    basis_high,
    basis_low,
    turned_high,
    turned_low,
    lift_high,
    lift_low,
    lower_high,
    lower_low,
    gram_high,
    gram_low,
    jump_high,
    jump_low,
    points_up,
    vec_up,
    product_out,
    product_in,
    line_1,
    cross_1,
    line_2,
    cross_2_out,
    cross_2_in,
    top_3,
    line_1b,
    cross_1b,
    line_2b,
    cross_2b_out,
    cross_2b_in,
    top_3b,
    sums_1,
    sums_2,
    sums_3,
    load_sem,
    send_sem,
    recv_sem,
):
    groups, n_x, n_y, n_core = sizes
    n_cross = n_x * n_core
    boxes = n_cross * n_y
    grp, pos_x, pos_y, pos_core = (lax.axis_index(name) for name in GRP_LEAF)
    box = (pos_x * n_y + pos_y) * n_core + pos_core
    cross = pos_x * n_core + pos_core

    def along_line(step):
        return (grp, pos_x, lax.rem(pos_y + step + n_y, n_y), pos_core)

    def along_cross(step):
        other = lax.rem(cross + step + n_cross, n_cross)
        return (grp, other // n_core, pos_y, lax.rem(other, n_core))

    def along_groups(step):
        return (lax.rem(grp + step + groups, groups), pos_x, pos_y, pos_core)

    def along_boxes(step):
        other = lax.rem(box + step + boxes, boxes)
        return (
            grp,
            other // (n_y * n_core),
            lax.rem(other // n_core, n_y),
            lax.rem(other, n_core),
        )

    loads = {}
    for index, (name, source, target) in enumerate(
        (
            ("rhs", rhs_hbm, rhs_ref),
            ("basis", basis_hbm, basis_ref),
            ("lift", lift_hbm, lift_ref),
            ("points", points_hbm, points_ref),
            ("scale", scale_hbm, scale_ref),
            ("leaf_skel", leaf_skel_hbm, leaf_skel_ref),
            ("group_skel", group_skel_hbm, group_skel_ref),
            ("links", links_hbm, links_ref),
            ("noise", noise_hbm, noise_ref),
        )
    ):
        loads[name] = pltpu.make_async_copy(source, target, load_sem.at[index])
        loads[name].start()

    barrier = pltpu.get_barrier_semaphore()
    partners = [along_groups(step) for step in range(1, groups)]
    partners += [along_line(step) for step in range(1, n_y)]
    partners += [along_cross(step) for step in range(1, n_cross)]
    partners += [along_boxes(-1), along_boxes(1)]
    for partner in partners:
        pl.semaphore_signal(barrier, inc=1, device_id=partner, device_id_type=MESH)

    started = []

    def send(source, target, device):
        index = len(started)
        copy = pltpu.make_async_remote_copy(
            src_ref=source,
            dst_ref=target,
            send_sem=send_sem.at[index],
            recv_sem=recv_sem.at[index],
            device_id=device,
            device_id_type=MESH,
        )
        copy.start()
        started.append(copy)
        return copy

    def spread(buffer, count, along):
        order = sorted(range(1, count), key=lambda step: -min(step, count - step))
        return [send(buffer.at[0], buffer.at[step], along(step)) for step in order]

    def arrived(copies):
        for copy in copies:
            copy.wait_recv()

    def keep(value, high_ref, low_ref):
        high_ref[...], low_ref[...] = two_parts(value)

    for load in loads.values():
        load.wait()
    rhs = rhs_ref[...]
    keep(basis_ref[...], basis_high, basis_low)
    coeff = product(rhs, basis_high[...], basis_low[...])
    keep(lift_ref[0], lift_high, lift_low)
    lifted = product(coeff, lift_high[...], lift_low[...])
    diagonal = row_of((8, 8)) == lane_of((8, 8))
    inv_column = jnp.sum(jnp.where(diagonal, scale_ref[...], 0.0), axis=1, keepdims=True) * STRETCH
    own = points_ref[...] * inv_column
    width = own.shape[1]
    picked = jnp.where(row_of((width, 128)) == leaf_skel_ref[...], 1.0, 0.0).astype(BF16)
    parts = times(jnp.concatenate(three_parts(own), axis=0).astype(BF16), picked)
    skel = parts[:8] + (parts[8:16] + parts[16:])
    held = jnp.where(row_of((128, 128)) == group_skel_ref[...] - box * 128, 1.0, 0.0).astype(BF16)
    parts = times(jnp.concatenate(three_parts(skel), axis=0).astype(BF16), held)
    top_part = parts[:8] + (parts[8:16] + parts[16:])
    cross_1[0, :16, :] = lifted
    cross_1[0, 16:24, :] = skel
    cross_1[0, 24:, :] = top_part
    line_1[0, :16, :] = coeff
    line_1[0, 16:, :] = skel

    pl.semaphore_wait(barrier, len(partners))
    cross_1_copies = spread(cross_1, n_cross, along_cross)
    line_1_copies = spread(line_1, n_y, along_line)
    points_copy = send(points_ref, points_up, along_boxes(-1))
    vec_copy = send(rhs_ref, vec_up.at[0], along_boxes(-1))

    right_bit = links_ref[:, 1:2].astype(F32)
    weight_self = 1.0 + links_ref[:, 0:1].astype(F32) + right_bit
    left_ref[...] = features(own, True).T.astype(BF16)
    right_ref[...] = features(own, False).astype(BF16)
    fill_block(left_ref, right_ref, self_high, self_low)

    arrived(cross_1_copies)
    line_2[0, :16, :] = added_up(cross_1, n_cross, 0, 16)
    line_2[0, 16:, :] = added_up(cross_1, n_cross, 24, 32)
    line_2_copies = spread(line_2, n_y, along_line)

    arrived([points_copy, vec_copy])
    right_ref[...] = features(points_up[...] * inv_column, False).astype(BF16)
    fill_block(left_ref, right_ref, link_high, link_low)
    product_out[0] = right_bit * product(rhs, link_high[...], link_low[...])
    product_copy = send(product_out.at[0], product_in.at[0], along_boxes(1))

    arrived(line_1_copies)
    far_left = features(side_by_side(line_1, n_y, 16, 24), True).T
    left_ref[: n_y * 128, :] = far_left.astype(BF16)
    far_right = features(side_by_side(cross_1, n_cross, 16, 24), False)
    right_ref[:, : n_cross * 128] = far_right.astype(BF16)
    middle = n_y * 64
    fill_block(left_ref, right_ref, far_high, far_low, bottom=middle)

    arrived(line_2_copies)
    top_3[0, :16, :] = added_up(line_2, n_y, 0, 16)
    top_own = added_up(line_2, n_y, 16, 24)
    top_3[0, 16:, :] = top_own
    top_3_copies = spread(top_3, groups, along_groups)
    fill_block(left_ref, right_ref, far_high, far_low, top=middle)

    def far_terms(spread_out, out, into):
        for slot in range(n_cross):
            out[slot] = spread_out[:, slot * 128 : (slot + 1) * 128]
        order = sorted(range(1, n_cross), key=lambda step: -min(step, n_cross - step))
        return [send(out.at[slot], into.at[slot], along_cross(-slot)) for slot in order]

    def far_sum(out, into):
        total = out[0]
        for slot in range(1, n_cross):
            total = total + into[slot]
        return total

    line_coeff = side_by_side(line_1, n_y, 0, 16)
    cross_2_copies = far_terms(
        product(line_coeff, far_high[...], far_low[...]), cross_2_out, cross_2_in
    )

    noise = noise_ref[...]

    def self_part(vec):
        return noise * vec + weight_self * product(vec, self_high[...], self_low[...])

    def upper_part(above):
        return right_bit * product(above, link_high[...], link_low[...], True)

    near = self_part(rhs) + upper_part(vec_up[0])

    turned = basis_ref[...].T
    keep(turned, turned_high, turned_low)
    gram = product(turned, basis_high[...], basis_low[...])
    both = jnp.concatenate([gram, product(gram, lift_high[...], lift_low[...])], axis=1)
    keep(both, gram_high, gram_low)
    lower = lift_ref[0].T
    keep(lower, lower_high, lower_low)
    keep(product(lower, gram_high[...], gram_low[...]), jump_high, jump_low)
    dot_rr = lane_sum(rhs * rhs)

    arrived([product_copy])
    near = near + product_in[0]
    image_ref[...] = near
    near_coeff = product(near, basis_high[...], basis_low[...])
    known = jnp.concatenate(
        [near_coeff, product(near_coeff, lift_high[...], lift_low[...])], axis=1
    )
    arrived(cross_2_copies)
    far = far_sum(cross_2_out, cross_2_in)
    known = known + product(far, gram_high[...], gram_low[...])
    top_right_ref[:, :128] = features(top_own, False).astype(BF16)

    arrived(top_3_copies)
    top_all = side_by_side(top_3, groups, 16, 24)
    top_left_ref[...] = features(top_all, True).T.astype(BF16)
    fill_block(top_left_ref, top_right_ref, top_high, top_low, 0, 128)
    top = product(side_by_side(top_3, groups, 0, 16), top_high[:, :128], top_low[:, :128])
    both = known + product(top, jump_high[...], jump_low[...])
    coeff = both[:, :128]
    cross_1b[0, :16, :] = both[:, 128:]
    cross_1b[0, 16:, :] = coeff
    line_1b[0] = coeff
    line_1b_copies = spread(line_1b, n_y, along_line)
    cross_1b_copies = spread(cross_1b, n_cross, along_cross)
    row = far + product(top, lower_high[...], lower_low[...])
    image = image_ref[...] + product(row, turned_high[...], turned_low[...])
    image_ref[...] = image
    vec_copy = send(image_ref, vec_up.at[1], along_boxes(-1))
    product_out[1] = right_bit * product(image, link_high[...], link_low[...])
    product_copy = send(product_out.at[1], product_in.at[1], along_boxes(1))
    near = self_part(image)
    dot_rw = lane_sum(rhs * image)
    dot_ww = lane_sum(image * image)
    dot_wu = lane_sum(image * near)
    arrived(cross_1b_copies)
    line_2b[0] = added_up(cross_1b, n_cross, 0, 16)
    line_2b_copies = spread(line_2b, n_y, along_line)
    arrived([vec_copy])
    upper = upper_part(vec_up[1])
    dot_wu = dot_wu + 2.0 * lane_sum(image * upper)
    second_ref[...] = near + upper
    arrived(line_1b_copies)
    spread_out = product(side_by_side(line_1b, n_y, 0, 16), far_high[...], far_low[...])
    cross_2b_copies = far_terms(spread_out, cross_2b_out, cross_2b_in)
    dot_wu = dot_wu + lane_sum(spread_out * side_by_side(cross_1b, n_cross, 16, 32))

    lane = lane_of((8, 128))
    packed = jnp.zeros((8, 128), F32)
    for index, dot in enumerate((dot_rr, dot_rw, dot_ww, dot_wu)):
        packed = jnp.where(lane == index, dot[:8], packed)
        packed = jnp.where(lane == index + 4, dot[8:], packed)
    sums_1[0] = packed
    sums_1_copies = spread(sums_1, n_cross, along_cross)

    top_right_ref[...] = features(top_all, False).astype(BF16)
    fill_block(top_left_ref, top_right_ref, top_high, top_low, 128)

    arrived(line_2b_copies)
    top_3b[0] = added_up(line_2b, n_y, 0, 16)
    top_3b_copies = spread(top_3b, groups, along_groups)
    arrived(sums_1_copies)
    sums_2[0] = added_up(sums_1, n_cross, 0, 8)
    sums_2_copies = spread(sums_2, n_y, along_line)
    arrived([product_copy])
    arrived(cross_2b_copies)
    far = far_sum(cross_2b_out, cross_2b_in)
    arrived(sums_2_copies)
    sums_3[0] = added_up(sums_2, n_y, 0, 8)
    sums_3_copies = spread(sums_3, groups, along_groups)
    arrived(top_3b_copies)
    top_coeff = side_by_side(top_3b, groups, 0, 16)
    top_out = product(top_coeff, top_high[...], top_low[...])
    row = far + product(top_out[:, :128], lower_high[...], lower_low[...])
    second_ref[...] = (
        second_ref[...] + product_in[1] + product(row, turned_high[...], turned_low[...])
    )
    top_wu = lane_sum(top_out * top_coeff)
    for copy in started:
        copy.wait_send()
    arrived(sums_3_copies)
    total = added_up(sums_3, groups, 0, 8)
    rr, rw, ww, wu = (
        jnp.concatenate([total[:, index : index + 1], total[:, index + 4 : index + 5]], axis=0)
        for index in range(4)
    )
    wu = wu + top_wu

    alpha = rr / rw
    next_rr = rr - 2.0 * alpha * rw + alpha * alpha * ww
    curve = rw - 2.0 * alpha * ww + alpha * alpha * wu
    ratio = next_rr / rr
    next_alpha = next_rr / (curve - ratio * next_rr / alpha)
    one_ref[...] = jnp.broadcast_to(alpha + next_alpha * (1.0 + ratio), one_ref.shape)
    two_ref[...] = jnp.broadcast_to(alpha * next_alpha, two_ref.shape)


def copies_of(sizes):
    groups, n_x, n_y, n_core = sizes
    n_cross = n_x * n_core
    return 5 * (n_y - 1) + 5 * (n_cross - 1) + 3 * (groups - 1) + 5


def local(sizes, points, rhs, basis, transfer, noise, inv_scale, links, leaf_skel, group_skel):
    groups, n_x, n_y, n_core = sizes
    n_cross = n_x * n_core
    width = points.shape[1]
    rows = rhs.shape[0]
    skel = leaf_skel.shape[1]
    count = copies_of(sizes)
    operands = (
        points,
        rhs,
        basis,
        transfer,
        noise[None, :],
        inv_scale[None, :],
        links,
        leaf_skel,
        group_skel,
    )

    def held(*shape):
        return pltpu.VMEM(shape, F32)

    def halves(*shape):
        return [pltpu.VMEM(shape, BF16)] * 2

    scratch = [
        *[pltpu.VMEM(operand.shape, operand.dtype) for operand in operands],
        pltpu.VMEM((width, FEATURES), BF16),
        pltpu.VMEM((FEATURES, width), BF16),
        pltpu.VMEM((groups * skel, FEATURES), BF16),
        pltpu.VMEM((FEATURES, groups * skel), BF16),
        *halves(width, width),
        *halves(width, width),
        *halves(n_y * skel, n_cross * skel),
        *halves(groups * skel, groups * skel),
        *halves(width, skel),
        *halves(skel, width),
        *halves(skel, skel),
        *halves(skel, skel),
        *halves(skel, 2 * skel),
        *halves(skel, 2 * skel),
        held(8, width),
        held(2, rows, width),
        held(2, rows, width),
        held(2, rows, width),
        held(n_y, rows + 8, skel),
        held(n_cross, rows + 16, skel),
        held(n_y, rows + 8, skel),
        held(n_cross, rows, skel),
        held(n_cross, rows, skel),
        held(groups, rows + 8, skel),
        held(n_y, rows, skel),
        held(n_cross, 2 * rows, skel),
        held(n_y, rows, skel),
        held(n_cross, rows, skel),
        held(n_cross, rows, skel),
        held(groups, rows, skel),
        held(n_cross, 8, skel),
        held(n_y, 8, skel),
        held(groups, 8, skel),
        pltpu.SemaphoreType.DMA((len(operands),)),
        pltpu.SemaphoreType.DMA((count,)),
        pltpu.SemaphoreType.DMA((count,)),
    ]
    vmem = pl.BlockSpec(memory_space=pltpu.VMEM)
    image, second, one, two = pl.pallas_call(
        functools.partial(everything, sizes),
        name="skeleton_cg",
        out_shape=[jax.ShapeDtypeStruct(rhs.shape, F32)] * 4,
        in_specs=[pl.BlockSpec(memory_space=pltpu.HBM)] * len(operands),
        out_specs=[vmem] * 4,
        scratch_shapes=scratch,
        compiler_params=pltpu.CompilerParams(
            collective_id=0, has_side_effects=True
        ),
    )(*operands)
    return one * rhs - two * image, rhs - one * image + two * second


def on_finer(finer):
    placed = (
        P(None, GRP_LEAF),
        P(None, GRP_LEAF),
        P(GRP_LEAF, None),
        P(GRP_LEAF, None, None),
        P(GRP_LEAF),
        P(),
        P(GRP_LEAF, None),
        P(GRP_LEAF, None),
        P("grp", None),
    )
    sizes = tuple(finer.shape[name] for name in GRP_LEAF)
    return jax.shard_map(
        functools.partial(local, sizes),
        mesh=finer,
        in_specs=placed,
        out_specs=(P(None, GRP_LEAF), P(None, GRP_LEAF)),
        check_vma=False,
    )


def solution(mesh):
    finer = Mesh(mesh.devices.reshape(mesh.shape["grp"], 4, 8, 2), GRP_LEAF)
    return on_finer(finer)
```

```python
import functools
import math

import jax
import jax.numpy as jnp
from jax import lax
from jax.experimental import pallas as pl
from jax.experimental.pallas import tpu as pltpu
from jax.sharding import Mesh
from jax.sharding import PartitionSpec as P

GRP_LEAF = ("grp", "leaf_0", "leaf_1", "leaf_2")
MESH = pl.DeviceIdType.MESH
F32 = jnp.float32
BF16 = jnp.bfloat16
FEATURES = 64
LN2 = math.log(2.0)
STRETCH = math.sqrt(5.0) / LN2


def row_of(shape):
    return lax.broadcasted_iota(jnp.int32, shape, 0)


def lane_of(shape):
    return lax.broadcasted_iota(jnp.int32, shape, 1)


def two_parts(value):
    high = value.astype(BF16)
    return high, (value - high.astype(F32)).astype(BF16)


def three_parts(value):
    first = value.astype(BF16).astype(F32)
    rest = value - first
    second = rest.astype(BF16).astype(F32)
    return first, second, (rest - second).astype(BF16).astype(F32)


def features(points, left):
    high, mid, low = three_parts(points)
    norm = jnp.sum(points * points, axis=0, keepdims=True)
    n_high, n_mid, n_low = three_parts(norm)
    row = row_of(points.shape)
    base = 0 if left else 3
    ones = (row >= 3) & (row < 6) if left else row < 3
    norms = jnp.where(
        row == base,
        n_high,
        jnp.where(
            row == base + 1, n_mid, jnp.where(row == base + 2, n_low, jnp.where(ones, 1.0, 0.0))
        ),
    )
    if left:
        two_high, two_mid, two_low = -2.0 * high, -2.0 * mid, -2.0 * low
        pieces = [two_high, two_high, two_mid, two_mid, two_high, two_low]
    else:
        pieces = [high, mid, high, mid, low, high]
    return jnp.concatenate(pieces + [norms, jnp.zeros_like(norms)], axis=0)


def kernel_values(left, right):
    dist = jnp.maximum(jnp.dot(left, right, preferred_element_type=F32), 1e-30)
    scaled = dist * lax.rsqrt(dist)
    return (1.0 + scaled * (LN2 + scaled * (LN2 * LN2 / 3.0))) * jnp.exp2(-scaled)


def fill_block(left_ref, right_ref, high_ref, low_ref, first=0, last=None, top=0, bottom=None):
    last = high_ref.shape[1] if last is None else last
    bottom = high_ref.shape[0] if bottom is None else bottom
    wide = min(256, last - first)
    tall = min(bottom - top, 1024 if last - first <= 128 else 512)

    def one(index, carry):
        at = pl.ds(pl.multiple_of(top + index * tall, tall), tall)
        left = left_ref[at, :]
        for start in range(first, last, wide):
            stop = min(start + wide, last)
            values = kernel_values(left, right_ref[:, start:stop])
            high, low = two_parts(values)
            high_ref[at, start:stop] = high
            low_ref[at, start:stop] = low
        return carry

    lax.fori_loop(0, (bottom - top) // tall, one, 0)


def times(first, second, turned=False):
    dims = (((1,), (1 if turned else 0,)), ((), ()))
    return lax.dot_general(first, second, dims, preferred_element_type=F32)


def product(vec, high, low, turned=False):
    vec_high, vec_low = two_parts(vec)
    rows = vec.shape[0]
    both = times(jnp.concatenate([vec_high, vec_low], axis=0), high, turned)
    return both[:rows] + (both[rows:] + times(vec_high, low, turned))


def side_by_side(buffer, count, start, stop):
    return jnp.concatenate([buffer[slot, start:stop, :] for slot in range(count)], axis=1)


def added_up(buffer, count, start, stop):
    total = buffer[0, start:stop, :]
    for slot in range(1, count):
        total = total + buffer[slot, start:stop, :]
    return total


def lane_sum(value):
    width = value.shape[1]
    total = value[:, :128]
    for start in range(128, width, 128):
        total = total + value[:, start : start + 128]
    return jnp.sum(total, axis=1, keepdims=True)


def everything(
    sizes,
    points_hbm,
    rhs_hbm,
    basis_hbm,
    lift_hbm,
    noise_hbm,
    scale_hbm,
    links_hbm,
    leaf_skel_hbm,
    group_skel_hbm,
    image_ref,
    second_ref,
    one_ref,
    two_ref,
    points_ref,
    rhs_ref,
    basis_ref,
    lift_ref,
    noise_ref,
    scale_ref,
    links_ref,
    leaf_skel_ref,
    group_skel_ref,
    left_ref,
    right_ref,
    top_left_ref,
    top_right_ref,
    self_high,
    self_low,
    link_high,
    link_low,
    far_high,
    far_low,
    top_high,
    top_low,
    basis_high,
    basis_low,
    turned_high,
    turned_low,
    lift_high,
    lift_low,
    lower_high,
    lower_low,
    gram_high,
    gram_low,
    jump_high,
    jump_low,
    points_up,
    vec_up,
    product_out,
    product_in,
    line_1,
    cross_1,
    line_2,
    cross_2_out,
    cross_2_in,
    top_3,
    line_1b,
    cross_1b,
    line_2b,
    cross_2b_out,
    cross_2b_in,
    top_3b,
    sums_1,
    sums_2,
    sums_3,
    load_sem,
    send_sem,
    recv_sem,
):
    groups, n_x, n_y, n_core = sizes
    n_cross = n_x * n_core
    boxes = n_cross * n_y
    grp, pos_x, pos_y, pos_core = (lax.axis_index(name) for name in GRP_LEAF)
    box = (pos_x * n_y + pos_y) * n_core + pos_core
    cross = pos_x * n_core + pos_core

    def along_line(step):
        return (grp, pos_x, lax.rem(pos_y + step + n_y, n_y), pos_core)

    def along_cross(step):
        other = lax.rem(cross + step + n_cross, n_cross)
        return (grp, other // n_core, pos_y, lax.rem(other, n_core))

    def along_groups(step):
        return (lax.rem(grp + step + groups, groups), pos_x, pos_y, pos_core)

    def along_boxes(step):
        other = lax.rem(box + step + boxes, boxes)
        return (
            grp,
            other // (n_y * n_core),
            lax.rem(other // n_core, n_y),
            lax.rem(other, n_core),
        )

    loads = {}
    for index, (name, source, target) in enumerate(
        (
            ("rhs", rhs_hbm, rhs_ref),
            ("basis", basis_hbm, basis_ref),
            ("lift", lift_hbm, lift_ref),
            ("points", points_hbm, points_ref),
            ("scale", scale_hbm, scale_ref),
            ("leaf_skel", leaf_skel_hbm, leaf_skel_ref),
            ("group_skel", group_skel_hbm, group_skel_ref),
            ("links", links_hbm, links_ref),
            ("noise", noise_hbm, noise_ref),
        )
    ):
        loads[name] = pltpu.make_async_copy(source, target, load_sem.at[index])
        loads[name].start()

    barrier = pltpu.get_barrier_semaphore()
    partners = [along_groups(step) for step in range(1, groups)]
    partners += [along_line(step) for step in range(1, n_y)]
    partners += [along_cross(step) for step in range(1, n_cross)]
    partners += [along_boxes(-1), along_boxes(1)]
    for partner in partners:
        pl.semaphore_signal(barrier, inc=1, device_id=partner, device_id_type=MESH)

    started = []

    def send(source, target, device):
        index = len(started)
        copy = pltpu.make_async_remote_copy(
            src_ref=source,
            dst_ref=target,
            send_sem=send_sem.at[index],
            recv_sem=recv_sem.at[index],
            device_id=device,
            device_id_type=MESH,
        )
        copy.start()
        started.append(copy)
        return copy

    def spread(buffer, count, along):
        order = sorted(range(1, count), key=lambda step: -min(step, count - step))
        return [send(buffer.at[0], buffer.at[step], along(step)) for step in order]

    def arrived(copies):
        for copy in copies:
            copy.wait_recv()

    def keep(value, high_ref, low_ref):
        high_ref[...], low_ref[...] = two_parts(value)

    for load in loads.values():
        load.wait()
    rhs = rhs_ref[...]
    keep(basis_ref[...], basis_high, basis_low)
    coeff = product(rhs, basis_high[...], basis_low[...])
    keep(lift_ref[0], lift_high, lift_low)
    lifted = product(coeff, lift_high[...], lift_low[...])
    diagonal = row_of((8, 8)) == lane_of((8, 8))
    inv_column = jnp.sum(jnp.where(diagonal, scale_ref[...], 0.0), axis=1, keepdims=True) * STRETCH
    own = points_ref[...] * inv_column
    width = own.shape[1]
    picked = jnp.where(row_of((width, 128)) == leaf_skel_ref[...], 1.0, 0.0).astype(BF16)
    parts = times(jnp.concatenate(three_parts(own), axis=0).astype(BF16), picked)
    skel = parts[:8] + (parts[8:16] + parts[16:])
    held = jnp.where(row_of((128, 128)) == group_skel_ref[...] - box * 128, 1.0, 0.0).astype(BF16)
    parts = times(jnp.concatenate(three_parts(skel), axis=0).astype(BF16), held)
    top_part = parts[:8] + (parts[8:16] + parts[16:])
    cross_1[0, :16, :] = lifted
    cross_1[0, 16:24, :] = skel
    cross_1[0, 24:, :] = top_part
    line_1[0, :16, :] = coeff
    line_1[0, 16:, :] = skel

    pl.semaphore_wait(barrier, len(partners))
    cross_1_copies = spread(cross_1, n_cross, along_cross)
    points_copy = send(points_ref, points_up, along_boxes(-1))
    line_1_copies = spread(line_1, n_y, along_line)
    vec_copy = send(rhs_ref, vec_up.at[0], along_boxes(-1))

    right_bit = links_ref[:, 1:2].astype(F32)
    weight_self = 1.0 + links_ref[:, 0:1].astype(F32) + right_bit
    left_ref[...] = features(own, True).T.astype(BF16)
    right_ref[...] = features(own, False).astype(BF16)
    fill_block(left_ref, right_ref, self_high, self_low)

    arrived(cross_1_copies)
    line_2[0, :16, :] = added_up(cross_1, n_cross, 0, 16)
    line_2[0, 16:, :] = added_up(cross_1, n_cross, 24, 32)
    line_2_copies = spread(line_2, n_y, along_line)

    arrived([points_copy])
    right_ref[...] = features(points_up[...] * inv_column, False).astype(BF16)
    fill_block(left_ref, right_ref, link_high, link_low)
    product_out[0] = right_bit * product(rhs, link_high[...], link_low[...])
    product_copy = send(product_out.at[0], product_in.at[0], along_boxes(1))

    arrived(line_1_copies)
    far_left = features(side_by_side(line_1, n_y, 16, 24), True).T
    left_ref[: n_y * 128, :] = far_left.astype(BF16)
    far_right = features(side_by_side(cross_1, n_cross, 16, 24), False)
    right_ref[:, : n_cross * 128] = far_right.astype(BF16)
    middle = n_y * 64
    fill_block(left_ref, right_ref, far_high, far_low, bottom=middle)

    arrived(line_2_copies)
    top_3[0, :16, :] = added_up(line_2, n_y, 0, 16)
    top_own = added_up(line_2, n_y, 16, 24)
    top_3[0, 16:, :] = top_own
    top_3_copies = spread(top_3, groups, along_groups)
    fill_block(left_ref, right_ref, far_high, far_low, top=middle)

    def far_terms(spread_out, out, into):
        for slot in range(n_cross):
            out[slot] = spread_out[:, slot * 128 : (slot + 1) * 128]
        order = sorted(range(1, n_cross), key=lambda step: -min(step, n_cross - step))
        return [send(out.at[slot], into.at[slot], along_cross(-slot)) for slot in order]

    def far_sum(out, into):
        total = out[0]
        for slot in range(1, n_cross):
            total = total + into[slot]
        return total

    line_coeff = side_by_side(line_1, n_y, 0, 16)
    cross_2_copies = far_terms(
        product(line_coeff, far_high[...], far_low[...]), cross_2_out, cross_2_in
    )

    noise = noise_ref[...]

    def self_part(vec):
        return noise * vec + weight_self * product(vec, self_high[...], self_low[...])

    def upper_part(above):
        return right_bit * product(above, link_high[...], link_low[...], True)

    near = self_part(rhs)
    arrived([vec_copy])
    near = near + upper_part(vec_up[0])

    turned = basis_ref[...].T
    keep(turned, turned_high, turned_low)
    gram = product(turned, basis_high[...], basis_low[...])
    both = jnp.concatenate([gram, product(gram, lift_high[...], lift_low[...])], axis=1)
    keep(both, gram_high, gram_low)
    lower = lift_ref[0].T
    keep(lower, lower_high, lower_low)
    keep(product(lower, gram_high[...], gram_low[...]), jump_high, jump_low)
    dot_rr = lane_sum(rhs * rhs)

    arrived([product_copy])
    near = near + product_in[0]
    image_ref[...] = near
    near_coeff = product(near, basis_high[...], basis_low[...])
    known = jnp.concatenate(
        [near_coeff, product(near_coeff, lift_high[...], lift_low[...])], axis=1
    )
    arrived(cross_2_copies)
    far = far_sum(cross_2_out, cross_2_in)
    known = known + product(far, gram_high[...], gram_low[...])
    top_right_ref[:, :128] = features(top_own, False).astype(BF16)

    arrived(top_3_copies)
    top_all = side_by_side(top_3, groups, 16, 24)
    top_left_ref[...] = features(top_all, True).T.astype(BF16)
    fill_block(top_left_ref, top_right_ref, top_high, top_low, 0, 128)
    top = product(side_by_side(top_3, groups, 0, 16), top_high[:, :128], top_low[:, :128])
    both = known + product(top, jump_high[...], jump_low[...])
    coeff = both[:, :128]
    cross_1b[0, :16, :] = both[:, 128:]
    cross_1b[0, 16:, :] = coeff
    line_1b[0] = coeff
    line_1b_copies = spread(line_1b, n_y, along_line)
    cross_1b_copies = spread(cross_1b, n_cross, along_cross)
    row = far + product(top, lower_high[...], lower_low[...])
    image = image_ref[...] + product(row, turned_high[...], turned_low[...])
    image_ref[...] = image
    vec_copy = send(image_ref, vec_up.at[1], along_boxes(-1))
    product_out[1] = right_bit * product(image, link_high[...], link_low[...])
    product_copy = send(product_out.at[1], product_in.at[1], along_boxes(1))
    near = self_part(image)
    dot_rw = lane_sum(rhs * image)
    dot_ww = lane_sum(image * image)
    dot_wu = lane_sum(image * near)
    arrived(cross_1b_copies)
    line_2b[0] = added_up(cross_1b, n_cross, 0, 16)
    line_2b_copies = spread(line_2b, n_y, along_line)
    second_ref[...] = near
    arrived([vec_copy])
    dot_wu = dot_wu + 2.0 * lane_sum(product_out[1] * vec_up[1])
    arrived(line_1b_copies)
    spread_out = product(side_by_side(line_1b, n_y, 0, 16), far_high[...], far_low[...])
    cross_2b_copies = far_terms(spread_out, cross_2b_out, cross_2b_in)
    dot_wu = dot_wu + lane_sum(spread_out * side_by_side(cross_1b, n_cross, 16, 32))

    lane = lane_of((8, 128))
    packed = jnp.zeros((8, 128), F32)
    for index, dot in enumerate((dot_rr, dot_rw, dot_ww, dot_wu)):
        packed = jnp.where(lane == index, dot[:8], packed)
        packed = jnp.where(lane == index + 4, dot[8:], packed)
    sums_1[0] = packed
    sums_1_copies = spread(sums_1, n_cross, along_cross)
    second_ref[...] = second_ref[...] + upper_part(vec_up[1])

    top_right_ref[...] = features(top_all, False).astype(BF16)
    fill_block(top_left_ref, top_right_ref, top_high, top_low, 128)

    arrived(line_2b_copies)
    top_3b[0] = added_up(line_2b, n_y, 0, 16)
    top_3b_copies = spread(top_3b, groups, along_groups)
    arrived(sums_1_copies)
    sums_2[0] = added_up(sums_1, n_cross, 0, 8)
    sums_2_copies = spread(sums_2, n_y, along_line)
    arrived([product_copy])
    arrived(cross_2b_copies)
    far = far_sum(cross_2b_out, cross_2b_in)
    arrived(sums_2_copies)
    sums_3[0] = added_up(sums_2, n_y, 0, 8)
    sums_3_copies = spread(sums_3, groups, along_groups)
    arrived(top_3b_copies)
    top_coeff = side_by_side(top_3b, groups, 0, 16)
    top_out = product(top_coeff, top_high[...], top_low[...])
    row = far + product(top_out[:, :128], lower_high[...], lower_low[...])
    second_ref[...] = (
        second_ref[...] + product_in[1] + product(row, turned_high[...], turned_low[...])
    )
    top_wu = lane_sum(top_out * top_coeff)
    for copy in started:
        copy.wait_send()
    arrived(sums_3_copies)
    total = added_up(sums_3, groups, 0, 8)
    rr, rw, ww, wu = (
        jnp.concatenate([total[:, index : index + 1], total[:, index + 4 : index + 5]], axis=0)
        for index in range(4)
    )
    wu = wu + top_wu

    alpha = rr / rw
    next_rr = rr - 2.0 * alpha * rw + alpha * alpha * ww
    curve = rw - 2.0 * alpha * ww + alpha * alpha * wu
    ratio = next_rr / rr
    next_alpha = next_rr / (curve - ratio * next_rr / alpha)
    one_ref[...] = jnp.broadcast_to(alpha + next_alpha * (1.0 + ratio), one_ref.shape)
    two_ref[...] = jnp.broadcast_to(alpha * next_alpha, two_ref.shape)


def copies_of(sizes):
    groups, n_x, n_y, n_core = sizes
    n_cross = n_x * n_core
    return 5 * (n_y - 1) + 5 * (n_cross - 1) + 3 * (groups - 1) + 5


def local(sizes, points, rhs, basis, transfer, noise, inv_scale, links, leaf_skel, group_skel):
    groups, n_x, n_y, n_core = sizes
    n_cross = n_x * n_core
    width = points.shape[1]
    rows = rhs.shape[0]
    skel = leaf_skel.shape[1]
    count = copies_of(sizes)
    operands = (
        points,
        rhs,
        basis,
        transfer,
        noise[None, :],
        inv_scale[None, :],
        links,
        leaf_skel,
        group_skel,
    )

    def held(*shape):
        return pltpu.VMEM(shape, F32)

    def halves(*shape):
        return [pltpu.VMEM(shape, BF16)] * 2

    scratch = [
        *[pltpu.VMEM(operand.shape, operand.dtype) for operand in operands],
        pltpu.VMEM((width, FEATURES), BF16),
        pltpu.VMEM((FEATURES, width), BF16),
        pltpu.VMEM((groups * skel, FEATURES), BF16),
        pltpu.VMEM((FEATURES, groups * skel), BF16),
        *halves(width, width),
        *halves(width, width),
        *halves(n_y * skel, n_cross * skel),
        *halves(groups * skel, groups * skel),
        *halves(width, skel),
        *halves(skel, width),
        *halves(skel, skel),
        *halves(skel, skel),
        *halves(skel, 2 * skel),
        *halves(skel, 2 * skel),
        held(8, width),
        held(2, rows, width),
        held(2, rows, width),
        held(2, rows, width),
        held(n_y, rows + 8, skel),
        held(n_cross, rows + 16, skel),
        held(n_y, rows + 8, skel),
        held(n_cross, rows, skel),
        held(n_cross, rows, skel),
        held(groups, rows + 8, skel),
        held(n_y, rows, skel),
        held(n_cross, 2 * rows, skel),
        held(n_y, rows, skel),
        held(n_cross, rows, skel),
        held(n_cross, rows, skel),
        held(groups, rows, skel),
        held(n_cross, 8, skel),
        held(n_y, 8, skel),
        held(groups, 8, skel),
        pltpu.SemaphoreType.DMA((len(operands),)),
        pltpu.SemaphoreType.DMA((count,)),
        pltpu.SemaphoreType.DMA((count,)),
    ]
    vmem = pl.BlockSpec(memory_space=pltpu.VMEM)
    image, second, one, two = pl.pallas_call(
        functools.partial(everything, sizes),
        name="skeleton_cg",
        out_shape=[jax.ShapeDtypeStruct(rhs.shape, F32)] * 4,
        in_specs=[pl.BlockSpec(memory_space=pltpu.HBM)] * len(operands),
        out_specs=[vmem] * 4,
        scratch_shapes=scratch,
        compiler_params=pltpu.CompilerParams(
            collective_id=0, has_side_effects=True
        ),
    )(*operands)
    return one * rhs - two * image, rhs - one * image + two * second


def on_finer(finer):
    placed = (
        P(None, GRP_LEAF),
        P(None, GRP_LEAF),
        P(GRP_LEAF, None),
        P(GRP_LEAF, None, None),
        P(GRP_LEAF),
        P(),
        P(GRP_LEAF, None),
        P(GRP_LEAF, None),
        P("grp", None),
    )
    sizes = tuple(finer.shape[name] for name in GRP_LEAF)
    return jax.shard_map(
        functools.partial(local, sizes),
        mesh=finer,
        in_specs=placed,
        out_specs=(P(None, GRP_LEAF), P(None, GRP_LEAF)),
        check_vma=False,
    )


def solution(mesh):
    finer = Mesh(mesh.devices.reshape(mesh.shape["grp"], 4, 8, 2), GRP_LEAF)
    return on_finer(finer)
```

```python
import functools
import math

import jax
import jax.numpy as jnp
from jax import lax
from jax.experimental import pallas as pl
from jax.experimental.pallas import tpu as pltpu
from jax.sharding import Mesh
from jax.sharding import PartitionSpec as P

GRP_LEAF = ("grp", "leaf_0", "leaf_1", "leaf_2")
MESH = pl.DeviceIdType.MESH
F32 = jnp.float32
BF16 = jnp.bfloat16
FEATURES = 64
LN2 = math.log(2.0)
STRETCH = math.sqrt(5.0) / LN2


def row_of(shape):
    return lax.broadcasted_iota(jnp.int32, shape, 0)


def lane_of(shape):
    return lax.broadcasted_iota(jnp.int32, shape, 1)


def two_parts(value):
    high = value.astype(BF16)
    return high, (value - high.astype(F32)).astype(BF16)


def three_parts(value):
    first = value.astype(BF16).astype(F32)
    rest = value - first
    second = rest.astype(BF16).astype(F32)
    return first, second, (rest - second).astype(BF16).astype(F32)


def features(points, left):
    high, mid, low = three_parts(points)
    norm = jnp.sum(points * points, axis=0, keepdims=True)
    n_high, n_mid, n_low = three_parts(norm)
    row = row_of(points.shape)
    base = 0 if left else 3
    ones = (row >= 3) & (row < 6) if left else row < 3
    norms = jnp.where(
        row == base,
        n_high,
        jnp.where(
            row == base + 1, n_mid, jnp.where(row == base + 2, n_low, jnp.where(ones, 1.0, 0.0))
        ),
    )
    if left:
        two_high, two_mid, two_low = -2.0 * high, -2.0 * mid, -2.0 * low
        pieces = [two_high, two_high, two_mid, two_mid, two_high, two_low]
    else:
        pieces = [high, mid, high, mid, low, high]
    return jnp.concatenate(pieces + [norms, jnp.zeros_like(norms)], axis=0)


def kernel_values(left, right):
    dist = jnp.maximum(jnp.dot(left, right, preferred_element_type=F32), 1e-30)
    scaled = dist * lax.rsqrt(dist)
    return (1.0 + scaled * (LN2 + scaled * (LN2 * LN2 / 3.0))) * jnp.exp2(-scaled)


def fill_block(left_ref, right_ref, high_ref, low_ref, first=0, last=None, top=0, bottom=None):
    last = high_ref.shape[1] if last is None else last
    bottom = high_ref.shape[0] if bottom is None else bottom
    wide = min(256, last - first)
    tall = min(bottom - top, 1024 if last - first <= 128 else 512)

    def one(index, carry):
        at = pl.ds(pl.multiple_of(top + index * tall, tall), tall)
        left = left_ref[at, :]
        for start in range(first, last, wide):
            stop = min(start + wide, last)
            values = kernel_values(left, right_ref[:, start:stop])
            high, low = two_parts(values)
            high_ref[at, start:stop] = high
            low_ref[at, start:stop] = low
        return carry

    lax.fori_loop(0, (bottom - top) // tall, one, 0)


def times(first, second, turned=False):
    dims = (((1,), (1 if turned else 0,)), ((), ()))
    return lax.dot_general(first, second, dims, preferred_element_type=F32)


def product(vec, high, low, turned=False):
    vec_high, vec_low = two_parts(vec)
    rows = vec.shape[0]
    both = times(jnp.concatenate([vec_high, vec_low], axis=0), high, turned)
    return both[:rows] + (both[rows:] + times(vec_high, low, turned))


def side_by_side(buffer, count, start, stop):
    return jnp.concatenate([buffer[slot, start:stop, :] for slot in range(count)], axis=1)


def added_up(buffer, count, start, stop):
    total = buffer[0, start:stop, :]
    for slot in range(1, count):
        total = total + buffer[slot, start:stop, :]
    return total


def lane_sum(value):
    width = value.shape[1]
    total = value[:, :128]
    for start in range(128, width, 128):
        total = total + value[:, start : start + 128]
    return jnp.sum(total, axis=1, keepdims=True)


def everything(
    sizes,
    points_hbm,
    rhs_hbm,
    basis_hbm,
    lift_hbm,
    noise_hbm,
    scale_hbm,
    links_hbm,
    leaf_skel_hbm,
    group_skel_hbm,
    image_hbm,
    second_hbm,
    one_hbm,
    two_hbm,
    image_ref,
    second_ref,
    one_ref,
    two_ref,
    points_ref,
    rhs_ref,
    basis_ref,
    lift_ref,
    noise_ref,
    scale_ref,
    links_ref,
    leaf_skel_ref,
    group_skel_ref,
    left_ref,
    right_ref,
    top_left_ref,
    top_right_ref,
    self_high,
    self_low,
    link_high,
    link_low,
    far_high,
    far_low,
    top_high,
    top_low,
    basis_high,
    basis_low,
    turned_high,
    turned_low,
    lift_high,
    lift_low,
    lower_high,
    lower_low,
    gram_high,
    gram_low,
    jump_high,
    jump_low,
    points_up,
    vec_up,
    product_out,
    product_in,
    line_1,
    cross_1,
    line_2,
    cross_2_out,
    cross_2_in,
    top_3,
    line_1b,
    cross_1b,
    line_2b,
    cross_2b_out,
    cross_2b_in,
    top_3b,
    sums_1,
    sums_2,
    sums_3,
    load_sem,
    send_sem,
    recv_sem,
):
    groups, n_x, n_y, n_core = sizes
    n_cross = n_x * n_core
    boxes = n_cross * n_y
    grp, pos_x, pos_y, pos_core = (lax.axis_index(name) for name in GRP_LEAF)
    box = (pos_x * n_y + pos_y) * n_core + pos_core
    cross = pos_x * n_core + pos_core

    def along_line(step):
        return (grp, pos_x, lax.rem(pos_y + step + n_y, n_y), pos_core)

    def along_cross(step):
        other = lax.rem(cross + step + n_cross, n_cross)
        return (grp, other // n_core, pos_y, lax.rem(other, n_core))

    def along_groups(step):
        return (lax.rem(grp + step + groups, groups), pos_x, pos_y, pos_core)

    def along_boxes(step):
        other = lax.rem(box + step + boxes, boxes)
        return (
            grp,
            other // (n_y * n_core),
            lax.rem(other // n_core, n_y),
            lax.rem(other, n_core),
        )

    loads = {}
    for index, (name, source, target) in enumerate(
        (
            ("rhs", rhs_hbm, rhs_ref),
            ("basis", basis_hbm, basis_ref),
            ("lift", lift_hbm, lift_ref),
            ("points", points_hbm, points_ref),
            ("scale", scale_hbm, scale_ref),
            ("leaf_skel", leaf_skel_hbm, leaf_skel_ref),
            ("group_skel", group_skel_hbm, group_skel_ref),
            ("links", links_hbm, links_ref),
            ("noise", noise_hbm, noise_ref),
        )
    ):
        loads[name] = pltpu.make_async_copy(source, target, load_sem.at[index])
        loads[name].start()

    barrier = pltpu.get_barrier_semaphore()
    partners = [along_groups(step) for step in range(1, groups)]
    partners += [along_line(step) for step in range(1, n_y)]
    partners += [along_cross(step) for step in range(1, n_cross)]
    partners += [along_boxes(-1), along_boxes(1)]
    for partner in partners:
        pl.semaphore_signal(barrier, inc=1, device_id=partner, device_id_type=MESH)

    started = []

    def send(source, target, device):
        index = len(started)
        copy = pltpu.make_async_remote_copy(
            src_ref=source,
            dst_ref=target,
            send_sem=send_sem.at[index],
            recv_sem=recv_sem.at[index],
            device_id=device,
            device_id_type=MESH,
        )
        copy.start()
        started.append(copy)
        return copy

    def spread(buffer, count, along):
        order = sorted(range(1, count), key=lambda step: -min(step, count - step))
        return [send(buffer.at[0], buffer.at[step], along(step)) for step in order]

    def arrived(copies):
        for copy in copies:
            copy.wait_recv()

    def keep(value, high_ref, low_ref):
        high_ref[...], low_ref[...] = two_parts(value)

    for load in loads.values():
        load.wait()
    rhs = rhs_ref[...]
    keep(basis_ref[...], basis_high, basis_low)
    coeff = product(rhs, basis_high[...], basis_low[...])
    keep(lift_ref[0], lift_high, lift_low)
    lifted = product(coeff, lift_high[...], lift_low[...])
    diagonal = row_of((8, 8)) == lane_of((8, 8))
    inv_column = jnp.sum(jnp.where(diagonal, scale_ref[...], 0.0), axis=1, keepdims=True) * STRETCH
    own = points_ref[...] * inv_column
    width = own.shape[1]
    picked = jnp.where(row_of((width, 128)) == leaf_skel_ref[...], 1.0, 0.0).astype(BF16)
    parts = times(jnp.concatenate(three_parts(own), axis=0).astype(BF16), picked)
    skel = parts[:8] + (parts[8:16] + parts[16:])
    held = jnp.where(row_of((128, 128)) == group_skel_ref[...] - box * 128, 1.0, 0.0).astype(BF16)
    parts = times(jnp.concatenate(three_parts(skel), axis=0).astype(BF16), held)
    top_part = parts[:8] + (parts[8:16] + parts[16:])
    cross_1[0, :16, :] = lifted
    cross_1[0, 16:24, :] = skel
    cross_1[0, 24:, :] = top_part
    line_1[0, :16, :] = coeff
    line_1[0, 16:, :] = skel

    pl.semaphore_wait(barrier, len(partners))
    cross_1_copies = spread(cross_1, n_cross, along_cross)
    points_copy = send(points_ref, points_up, along_boxes(-1))
    line_1_copies = spread(line_1, n_y, along_line)
    vec_copy = send(rhs_ref, vec_up.at[0], along_boxes(-1))

    right_bit = links_ref[:, 1:2].astype(F32)
    weight_self = 1.0 + links_ref[:, 0:1].astype(F32) + right_bit
    left_ref[...] = features(own, True).T.astype(BF16)
    right_ref[...] = features(own, False).astype(BF16)
    fill_block(left_ref, right_ref, self_high, self_low)

    arrived(cross_1_copies)
    line_2[0, :16, :] = added_up(cross_1, n_cross, 0, 16)
    line_2[0, 16:, :] = added_up(cross_1, n_cross, 24, 32)
    line_2_copies = spread(line_2, n_y, along_line)

    arrived([points_copy])
    right_ref[...] = features(points_up[...] * inv_column, False).astype(BF16)
    fill_block(left_ref, right_ref, link_high, link_low)
    product_out[0] = right_bit * product(rhs, link_high[...], link_low[...])
    product_copy = send(product_out.at[0], product_in.at[0], along_boxes(1))

    arrived(line_1_copies)
    far_left = features(side_by_side(line_1, n_y, 16, 24), True).T
    left_ref[: n_y * 128, :] = far_left.astype(BF16)
    far_right = features(side_by_side(cross_1, n_cross, 16, 24), False)
    right_ref[:, : n_cross * 128] = far_right.astype(BF16)
    middle = n_y * 64
    fill_block(left_ref, right_ref, far_high, far_low, bottom=middle)

    arrived(line_2_copies)
    top_3[0, :16, :] = added_up(line_2, n_y, 0, 16)
    top_own = added_up(line_2, n_y, 16, 24)
    top_3[0, 16:, :] = top_own
    top_3_copies = spread(top_3, groups, along_groups)
    fill_block(left_ref, right_ref, far_high, far_low, top=middle)

    def far_terms(spread_out, out, into):
        for slot in range(n_cross):
            out[slot] = spread_out[:, slot * 128 : (slot + 1) * 128]
        order = sorted(range(1, n_cross), key=lambda step: -min(step, n_cross - step))
        return [send(out.at[slot], into.at[slot], along_cross(-slot)) for slot in order]

    def far_sum(out, into):
        total = out[0]
        for slot in range(1, n_cross):
            total = total + into[slot]
        return total

    line_coeff = side_by_side(line_1, n_y, 0, 16)
    cross_2_copies = far_terms(
        product(line_coeff, far_high[...], far_low[...]), cross_2_out, cross_2_in
    )

    noise = noise_ref[...]

    def self_part(vec):
        return noise * vec + weight_self * product(vec, self_high[...], self_low[...])

    def upper_part(above):
        return right_bit * product(above, link_high[...], link_low[...], True)

    near = self_part(rhs)
    arrived([vec_copy])
    near = near + upper_part(vec_up[0])

    turned = basis_ref[...].T
    keep(turned, turned_high, turned_low)
    gram = product(turned, basis_high[...], basis_low[...])
    both = jnp.concatenate([gram, product(gram, lift_high[...], lift_low[...])], axis=1)
    keep(both, gram_high, gram_low)
    lower = lift_ref[0].T
    keep(lower, lower_high, lower_low)
    keep(product(lower, gram_high[...], gram_low[...]), jump_high, jump_low)
    dot_rr = lane_sum(rhs * rhs)

    arrived([product_copy])
    near = near + product_in[0]
    image_ref[...] = near
    near_coeff = product(near, basis_high[...], basis_low[...])
    known = jnp.concatenate(
        [near_coeff, product(near_coeff, lift_high[...], lift_low[...])], axis=1
    )
    arrived(cross_2_copies)
    far = far_sum(cross_2_out, cross_2_in)
    known = known + product(far, gram_high[...], gram_low[...])
    top_right_ref[:, :128] = features(top_own, False).astype(BF16)

    arrived(top_3_copies)
    top_all = side_by_side(top_3, groups, 16, 24)
    top_left_ref[...] = features(top_all, True).T.astype(BF16)
    fill_block(top_left_ref, top_right_ref, top_high, top_low, 0, 128)
    top = product(side_by_side(top_3, groups, 0, 16), top_high[:, :128], top_low[:, :128])
    both = known + product(top, jump_high[...], jump_low[...])
    coeff = both[:, :128]
    cross_1b[0, :16, :] = both[:, 128:]
    cross_1b[0, 16:, :] = coeff
    line_1b[0] = coeff
    line_1b_copies = spread(line_1b, n_y, along_line)
    cross_1b_copies = spread(cross_1b, n_cross, along_cross)
    row = far + product(top, lower_high[...], lower_low[...])
    image = image_ref[...] + product(row, turned_high[...], turned_low[...])
    image_ref[...] = image
    vec_copy = send(image_ref, vec_up.at[1], along_boxes(-1))
    image_out = pltpu.make_async_copy(image_ref, image_hbm, load_sem.at[9])
    image_out.start()
    product_out[1] = right_bit * product(image, link_high[...], link_low[...])
    product_copy = send(product_out.at[1], product_in.at[1], along_boxes(1))
    near = self_part(image)
    dot_rw = lane_sum(rhs * image)
    dot_ww = lane_sum(image * image)
    dot_wu = lane_sum(image * near)
    arrived(cross_1b_copies)
    line_2b[0] = added_up(cross_1b, n_cross, 0, 16)
    line_2b_copies = spread(line_2b, n_y, along_line)
    second_ref[...] = near
    arrived([vec_copy])
    dot_wu = dot_wu + 2.0 * lane_sum(product_out[1] * vec_up[1])
    arrived(line_1b_copies)
    spread_out = product(side_by_side(line_1b, n_y, 0, 16), far_high[...], far_low[...])
    cross_2b_copies = far_terms(spread_out, cross_2b_out, cross_2b_in)
    dot_wu = dot_wu + lane_sum(spread_out * side_by_side(cross_1b, n_cross, 16, 32))

    lane = lane_of((8, 128))
    packed = jnp.zeros((8, 128), F32)
    for index, dot in enumerate((dot_rr, dot_rw, dot_ww, dot_wu)):
        packed = jnp.where(lane == index, dot[:8], packed)
        packed = jnp.where(lane == index + 4, dot[8:], packed)
    sums_1[0] = packed
    sums_1_copies = spread(sums_1, n_cross, along_cross)
    second_ref[...] = second_ref[...] + upper_part(vec_up[1])

    top_right_ref[...] = features(top_all, False).astype(BF16)
    fill_block(top_left_ref, top_right_ref, top_high, top_low, 128)

    arrived(line_2b_copies)
    top_3b[0] = added_up(line_2b, n_y, 0, 16)
    top_3b_copies = spread(top_3b, groups, along_groups)
    arrived(sums_1_copies)
    sums_2[0] = added_up(sums_1, n_cross, 0, 8)
    sums_2_copies = spread(sums_2, n_y, along_line)
    arrived([product_copy])
    arrived(cross_2b_copies)
    far = far_sum(cross_2b_out, cross_2b_in)
    arrived(sums_2_copies)
    sums_3[0] = added_up(sums_2, n_y, 0, 8)
    sums_3_copies = spread(sums_3, groups, along_groups)
    arrived(top_3b_copies)
    top_coeff = side_by_side(top_3b, groups, 0, 16)
    top_out = product(top_coeff, top_high[...], top_low[...])
    row = far + product(top_out[:, :128], lower_high[...], lower_low[...])
    second_ref[...] = (
        second_ref[...] + product_in[1] + product(row, turned_high[...], turned_low[...])
    )
    second_out = pltpu.make_async_copy(second_ref, second_hbm, load_sem.at[10])
    second_out.start()
    top_wu = lane_sum(top_out * top_coeff)
    for copy in started:
        copy.wait_send()
    image_out.wait()
    second_out.wait()
    arrived(sums_3_copies)
    total = added_up(sums_3, groups, 0, 8)
    rr, rw, ww, wu = (
        jnp.concatenate([total[:, index : index + 1], total[:, index + 4 : index + 5]], axis=0)
        for index in range(4)
    )
    wu = wu + top_wu

    alpha = rr / rw
    next_rr = rr - 2.0 * alpha * rw + alpha * alpha * ww
    curve = rw - 2.0 * alpha * ww + alpha * alpha * wu
    ratio = next_rr / rr
    next_alpha = next_rr / (curve - ratio * next_rr / alpha)
    one_ref[...] = jnp.broadcast_to(alpha + next_alpha * (1.0 + ratio), one_ref.shape)
    one_out = pltpu.make_async_copy(one_ref, one_hbm, load_sem.at[11])
    one_out.start()
    two_ref[...] = jnp.broadcast_to(alpha * next_alpha, two_ref.shape)
    two_out = pltpu.make_async_copy(two_ref, two_hbm, load_sem.at[12])
    two_out.start()
    one_out.wait()
    two_out.wait()


def copies_of(sizes):
    groups, n_x, n_y, n_core = sizes
    n_cross = n_x * n_core
    return 5 * (n_y - 1) + 5 * (n_cross - 1) + 3 * (groups - 1) + 5


def local(sizes, points, rhs, basis, transfer, noise, inv_scale, links, leaf_skel, group_skel):
    groups, n_x, n_y, n_core = sizes
    n_cross = n_x * n_core
    width = points.shape[1]
    rows = rhs.shape[0]
    skel = leaf_skel.shape[1]
    count = copies_of(sizes)
    operands = (
        points,
        rhs,
        basis,
        transfer,
        noise[None, :],
        inv_scale[None, :],
        links,
        leaf_skel,
        group_skel,
    )

    def held(*shape):
        return pltpu.VMEM(shape, F32)

    def halves(*shape):
        return [pltpu.VMEM(shape, BF16)] * 2

    scratch = [
        *[held(rows, width)] * 4,
        *[pltpu.VMEM(operand.shape, operand.dtype) for operand in operands],
        pltpu.VMEM((width, FEATURES), BF16),
        pltpu.VMEM((FEATURES, width), BF16),
        pltpu.VMEM((groups * skel, FEATURES), BF16),
        pltpu.VMEM((FEATURES, groups * skel), BF16),
        *halves(width, width),
        *halves(width, width),
        *halves(n_y * skel, n_cross * skel),
        *halves(groups * skel, groups * skel),
        *halves(width, skel),
        *halves(skel, width),
        *halves(skel, skel),
        *halves(skel, skel),
        *halves(skel, 2 * skel),
        *halves(skel, 2 * skel),
        held(8, width),
        held(2, rows, width),
        held(2, rows, width),
        held(2, rows, width),
        held(n_y, rows + 8, skel),
        held(n_cross, rows + 16, skel),
        held(n_y, rows + 8, skel),
        held(n_cross, rows, skel),
        held(n_cross, rows, skel),
        held(groups, rows + 8, skel),
        held(n_y, rows, skel),
        held(n_cross, 2 * rows, skel),
        held(n_y, rows, skel),
        held(n_cross, rows, skel),
        held(n_cross, rows, skel),
        held(groups, rows, skel),
        held(n_cross, 8, skel),
        held(n_y, 8, skel),
        held(groups, 8, skel),
        pltpu.SemaphoreType.DMA((len(operands) + 4,)),
        pltpu.SemaphoreType.DMA((count,)),
        pltpu.SemaphoreType.DMA((count,)),
    ]
    image, second, one, two = pl.pallas_call(
        functools.partial(everything, sizes),
        name="skeleton_cg",
        out_shape=[jax.ShapeDtypeStruct(rhs.shape, F32)] * 4,
        in_specs=[pl.BlockSpec(memory_space=pltpu.HBM)] * len(operands),
        out_specs=[pl.BlockSpec(memory_space=pltpu.HBM)] * 4,
        scratch_shapes=scratch,
        compiler_params=pltpu.CompilerParams(
            collective_id=0, has_side_effects=True
        ),
    )(*operands)
    return one * rhs - two * image, rhs - one * image + two * second


def on_finer(finer):
    placed = (
        P(None, GRP_LEAF),
        P(None, GRP_LEAF),
        P(GRP_LEAF, None),
        P(GRP_LEAF, None, None),
        P(GRP_LEAF),
        P(),
        P(GRP_LEAF, None),
        P(GRP_LEAF, None),
        P("grp", None),
    )
    sizes = tuple(finer.shape[name] for name in GRP_LEAF)
    return jax.shard_map(
        functools.partial(local, sizes),
        mesh=finer,
        in_specs=placed,
        out_specs=(P(None, GRP_LEAF), P(None, GRP_LEAF)),
        check_vma=False,
    )


def solution(mesh):
    finer = Mesh(mesh.devices.reshape(mesh.shape["grp"], 4, 8, 2), GRP_LEAF)
    return on_finer(finer)
```
